32 devices in a mesh: row: 8 (over z, x), col: 4 (over y, core).
Axes of the slice: x: 2, y: 2, z: 4, core: 2. Of those that a mesh axis runs over, the one named last changes fastest.
Arguments:
- krylov_basis: float32 [4, 2, 3, 128, 128, 256], P(None, None, None, 'col', 'row'), may hold values from -50 to 50
- susceptibility: float32 [128, 128, 256], P('col', 'row'), may hold values from 0.1 to 1
- green_spectra: bfloat16 [6, 256, 256, 512], P(None, None, 'col', 'row'), may hold values from -3 to 3, as said below
Outputs:
- projections: float32 [4, 2, 2], replicated
- next_block: float32 [2, 3, 128, 128, 256], P(None, None, 'col', 'row')
- block_factor: float32 [2, 2], replicated
The draws below stay inside these ranges and needn't reach their ends.
Inputs may be any that keep to these rules, and one draw needn't show every extreme that they name: `green_spectra`: each of the six arrays is even on the padded grid: its value at (a, b, c) equals its value at ((-a) mod 256, (-b) mod 256, (-c) mod 512).
All inputs are finite; a program needn't handle non-finite values.
Results may differ from the reference program's by a relative error of at most 0.0003.
Values sent between devices are 32-bit elements; how exact they have to be, the bound alone decides.
A program may use at most 192 MiB of HBM per device.

```python
import math
import jax
import jax.numpy as jnp
from jax import lax

GX = 256
GY = 128
GZ = 128
NB = 4


def draw_krylov_basis(key, part):
    shared = jnp.clip(jax.random.normal(jax.random.fold_in(key, 12), (2, 3, GZ, GY, GX), jnp.float32), -6.0, 6.0)
    depths = (jnp.arange(GZ, dtype=jnp.float32) + 0.5) / GZ
    across = (jnp.arange(GY, dtype=jnp.float32) + 0.5) / GY
    envelope = (0.3 + depths[:, None] + across[None, :])[:, :, None]
    own = jnp.clip(jax.random.normal(jax.random.fold_in(key, 11), (NB, 2, 3, GZ, GY, GX), jnp.float32), -6.0, 6.0)
    return (own + shared) * (envelope * math.sqrt(0.5))


def draw_green_spectra(key, part):

    def one_entry(entry_key):
        raw = jnp.clip(jax.random.normal(entry_key, (2 * GZ, 2 * GY, 2 * GX), jnp.float32), -6.0, 6.0)
        mirrored = jnp.roll(jnp.flip(raw), (1, 1, 1), axis=(0, 1, 2))
        return (0.25 * (raw + mirrored)).astype(jnp.bfloat16)
    entry_keys = jax.random.split(jax.random.fold_in(key, 21), 6)
    return lax.map(one_entry, entry_keys)


def block_scale(stream_key, extent, cuts, low, high):
    def one(dim, blocks):
        draws = jax.random.uniform(jax.random.fold_in(jax.random.fold_in(stream_key, 6), dim), (blocks,), jnp.float32, low / len(cuts), high / len(cuts))
        return jnp.repeat(jnp.exp(draws), extent[dim] // blocks).reshape((-1,) + (1,) * (len(extent) - dim - 1))

    factor_of = one(*cuts[0])
    for cut in cuts[1:]:
        factor_of = factor_of * one(*cut)
    return factor_of


def setup_inputs(seed: int = 0) -> dict:
    key_list = jax.random.split(jax.random.key(seed), 4)
    return {
        "krylov_basis": draw_krylov_basis(jax.random.fold_in(key_list[3], 71), 0),
        "susceptibility": jnp.clip(jnp.exp(math.log(1.0) - 2.3025851 * jax.random.uniform(key_list[1], (GZ, GY, GX), jnp.float32) ** block_scale(key_list[1], (GZ, GY, GX), ((0, 4), (1, 8)), -0.2, 0.2)), 0.1, 1.0),
        "green_spectra": draw_green_spectra(jax.random.fold_in(key_list[3], 71), 0),
    }


highest = lax.Precision.HIGHEST
tensor_pairs = ((0, 3, 4), (3, 1, 5), (4, 5, 2))

def convolve(field, green_spectra):
    padded_shape = (2 * GZ, 2 * GY, 2 * GX)
    half_kernel = green_spectra[:, :, :, :GX + 1].astype(jnp.float32)
    spectra = jnp.fft.rfftn(field, s=padded_shape, axes=(1, 2, 3))
    results = []
    for member in range(3):
        chosen = tensor_pairs[member]
        mixed = half_kernel[chosen[0]] * spectra[0] + half_kernel[chosen[1]] * spectra[1] + half_kernel[chosen[2]] * spectra[2]
        full_field = jnp.fft.irfftn(mixed, s=padded_shape, axes=(0, 1, 2))
        results.append(full_field[:GZ, :GY, :GX])
    return jnp.stack(results)

def reference(krylov_basis, susceptibility, green_spectra):
    latest = krylov_basis[NB - 1]
    response = jnp.stack([convolve(latest[0], green_spectra), convolve(latest[1], green_spectra)])
    image = latest - susceptibility[None, None] * response
    entry_count = 3.0 * GX * GY * GZ
    flat_basis = krylov_basis.reshape(2 * NB, -1)
    flat_image = image.reshape(2, -1)
    coefficients = jnp.dot(flat_basis, flat_image.T, precision=highest) / entry_count
    projected = flat_image - jnp.dot(coefficients.T, flat_basis, precision=highest)
    gram = jnp.dot(projected, projected.T, precision=highest) / entry_count
    lead_norm = jnp.sqrt(gram[0, 0] + 1e-06)
    cross_term = gram[0, 1] / lead_norm
    tail_norm = jnp.sqrt(gram[1, 1] - cross_term * cross_term + 1e-06)
    first_column = projected[0] / lead_norm
    second_column = (projected[1] - cross_term * first_column) / tail_norm
    next_block = jnp.stack([first_column, second_column]).reshape(image.shape)
    block_factor = jnp.stack([jnp.stack([lead_norm, cross_term]), jnp.stack([jnp.zeros_like(lead_norm), tail_norm])])
    return (coefficients.reshape(NB, 2, 2), next_block, block_factor)
```

```python
import functools
import math

import jax
import jax.numpy as jnp
from jax import lax
from jax.experimental import pallas as pl
from jax.experimental.pallas import tpu as pltpu
from jax.sharding import PartitionSpec as P

fast = lax.Precision.HIGH
tensor_pairs = ((0, 3, 4), (3, 1, 5), (4, 5, 2))


def twiddle(count_in, count_out, period, orient, factor):
    row_index = lax.broadcasted_iota(jnp.int32, (count_in, count_out), 0)
    col_index = lax.broadcasted_iota(jnp.int32, (count_in, count_out), 1)
    phases = row_index * col_index % period
    angles = phases.astype(jnp.float32) * (2.0 * math.pi / period)
    cosine = jnp.cos(angles) * factor
    sines = jnp.sin(angles) * (orient * factor)
    return jnp.stack([jnp.stack([cosine, sines]), jnp.stack([-sines, cosine])])


def exchange_rows(blocks):
    return lax.all_to_all(blocks, "row", split_axis=0, concat_axis=0, tiled=True)


def exchange_cols(blocks):
    return lax.all_to_all(blocks, "col", split_axis=0, concat_axis=0, tiled=True)


def forward(source, table_x, table_y, table_z):
    local_z, local_y = source.shape[1:3]
    row_count, part_x = table_x.shape[-2:]
    col_count, part_y = table_y.shape[-2:]
    spectra = jnp.einsum("rzyx,rsxdl->dsyzl", source, table_x, precision=fast)
    spectra = spectra.reshape(row_count, 2, local_y, local_z * part_x)
    spectra = exchange_rows(spectra)
    spectra = spectra.transpose(1, 0, 2, 3).reshape(2, row_count * local_y, local_z, part_x)
    spectra = jnp.einsum("ryzl,rsyeq->eszql", spectra, table_y, precision=fast)
    spectra = spectra.reshape(col_count, 2, local_z, part_y * part_x)
    spectra = exchange_cols(spectra)
    spectra = spectra.transpose(1, 0, 2, 3).reshape(2, col_count * local_z, part_y * part_x)
    return jnp.einsum("rzb,rszk->skb", spectra, table_z, precision=fast)


def backward(spectra, back_x, back_y, back_z):
    row_count, part_x = back_x.shape[2:4]
    col_count, part_y, width = back_y.shape[2:]
    spectra = jnp.einsum("rkb,rskz->szb", spectra, back_z, precision=fast)
    local_z = spectra.shape[1] // col_count
    spectra = spectra.reshape(2, col_count, local_z, part_y * part_x).transpose(1, 0, 2, 3)
    spectra = exchange_cols(spectra)
    spectra = spectra.reshape(col_count, 2, local_z, part_y, part_x)
    spectra = jnp.einsum("erzql,rseqy->syzl", spectra, back_y, precision=fast)
    local_y = width // row_count
    spectra = spectra.reshape(2, row_count, local_y, local_z * part_x).transpose(1, 0, 2, 3)
    spectra = exchange_rows(spectra)
    spectra = spectra.reshape(row_count, 2, local_y, local_z, part_x)
    return jnp.einsum("dryzl,rsdlx->szyx", spectra, back_x, precision=fast)


def convolve(source, green_spectra):
    row_count = lax.axis_size("row")
    col_count = lax.axis_size("col")
    width_x = 2 * source.shape[-1]
    width_y = 2 * source.shape[-2] * row_count
    width_z = 2 * source.shape[-3] * col_count
    part_x = width_x // row_count
    part_y = width_y // col_count
    half_x, half_y, half_z = width_x // 2, width_y // 2, width_z // 2
    table_x = twiddle(half_x, width_x, width_x, -1.0, 1.0).reshape(2, 2, half_x, row_count, part_x)
    table_y = twiddle(half_y, width_y, width_y, -1.0, 1.0).reshape(2, 2, half_y, col_count, part_y)
    table_z = twiddle(half_z, width_z, width_z, -1.0, 1.0)
    spectra = [forward(source[:, c], table_x, table_y, table_z) for c in range(3)]
    coupling = green_spectra.astype(jnp.float32).reshape(6, width_z, part_y * part_x)
    back_z = twiddle(width_z, half_z, width_z, 1.0, 1.0)
    back_y = twiddle(width_y, half_y, width_y, 1.0, 1.0).reshape(2, 2, col_count, part_y, half_y)
    scaling = 1.0 / (width_x * width_y * width_z)
    back_x = twiddle(width_x, half_x, width_x, 1.0, scaling).reshape(2, 2, row_count, part_x, half_x)
    result = []
    for member in range(3):
        chosen = tensor_pairs[member]
        total = coupling[chosen[0]] * spectra[0]
        total = total + coupling[chosen[1]] * spectra[1]
        total = total + coupling[chosen[2]] * spectra[2]
        result.append(backward(total, back_x, back_y, back_z))
    return result


LANES = 128
SLABS = 4
MESH = pl.DeviceIdType.MESH


def split_parts(table, axis):
    high = lax.reduce_precision(table, 8, 7)
    low = (table - high).astype(jnp.bfloat16)
    high = high.astype(jnp.bfloat16)
    return jnp.concatenate([high, high, low], axis=axis)


def phase_pair(points, freqs, period):
    phases = points * freqs % period
    angles = phases.astype(jnp.float32) * (2.0 * math.pi / period)
    return jnp.cos(angles), jnp.sin(angles)


def left_tables(half):
    freqs = lax.broadcasted_iota(jnp.int32, (2 * half, half), 0)
    points = lax.broadcasted_iota(jnp.int32, (2 * half, half), 1)
    cosine, sine = phase_pair(points, freqs, 2 * half)
    ahead = jnp.concatenate([cosine, sine], axis=1)
    back = jnp.concatenate([cosine.T, -sine.T], axis=1)
    return split_parts(ahead, 1), split_parts(back, 1)


def line_tables(half_x, row_count, part_x, scaling):
    wide = part_x // 2
    shape = (half_x, 2, row_count // 2, 2, wide)
    points = lax.broadcasted_iota(jnp.int32, shape, 0)
    freqs = lax.broadcasted_iota(jnp.int32, shape, 1) * wide
    freqs = freqs + lax.broadcasted_iota(jnp.int32, shape, 2) * (2 * part_x)
    freqs = freqs + lax.broadcasted_iota(jnp.int32, shape, 3) * part_x
    freqs = freqs + lax.broadcasted_iota(jnp.int32, shape, 4)
    cosine, sine = phase_pair(points, freqs, 2 * half_x)
    upper = jnp.stack([cosine, -sine], axis=3)
    lower = jnp.stack([sine, cosine], axis=3)
    ahead = jnp.stack([upper, lower]).transpose(2, 0, 1, 3, 4, 5, 6)
    ahead = ahead.reshape(2, 2 * half_x, row_count * part_x)
    upper = jnp.stack([cosine, -sine], axis=3)
    lower = jnp.stack([sine, cosine], axis=3)
    back = jnp.stack([upper, lower]).transpose(2, 3, 4, 5, 6, 0, 1)
    back = back.reshape(2 * row_count * part_x, 2 * half_x) * scaling
    return split_parts(ahead, 1), split_parts(back, 0)


def swap_lanes(first, second):
    last = first.ndim - 1
    lane = lax.broadcasted_iota(jnp.int32, first.shape, last)
    keep = lane % 64 < 32
    return (
        jnp.where(keep, first, pltpu.roll(second, 32, last)),
        jnp.where(keep, pltpu.roll(first, 96, last), second),
    )


def stacked_operand(column):
    lane = lax.broadcasted_iota(jnp.int32, column.shape, 1)
    turned = pltpu.roll(column, 64, 1)
    turned = jnp.where(lane < 64, turned, -turned)
    both = jnp.concatenate([column, turned], axis=0)
    high = both.astype(jnp.bfloat16)
    low = (both - high.astype(jnp.float32)).astype(jnp.bfloat16)
    return jnp.concatenate([high, low, high], axis=0)


def left_product(table, columns):
    operand = jnp.concatenate([stacked_operand(column) for column in columns], axis=1)
    return jnp.dot(table, operand, preferred_element_type=jnp.float32)


def right_product(rows, table):
    high = rows.astype(jnp.bfloat16)
    low = (rows - high.astype(jnp.float32)).astype(jnp.bfloat16)
    operand = jnp.concatenate([high, low, high], axis=1)
    return jnp.dot(operand, table, preferred_element_type=jnp.float32)


def field_kernel(
    row_count,
    col_count,
    krylov,
    chi,
    green,
    ahead_x,
    back_x,
    ahead_y,
    back_y,
    ahead_z,
    back_z,
    image,
    grid_a,
    grid_b,
    grid_c,
    grid_d,
    green_slot,
    green_wide,
    source_slot,
    chi_slot,
    image_slot,
    mixed,
    f1s, f1r, f1l, f2s, f2r, f2l, b1s, b1r, b1l, b2s, b2r, b2l,
    green_sem,
    source_sem,
    chi_sem,
    image_sem,
    row_credit,
    col_credit,
):
    blocks = krylov.shape[0]
    local_z, local_y, half_x = chi.shape
    pairs_y = grid_c.shape[4]
    full_z = green.shape[1]
    depth = local_z // SLABS
    pair_depth = depth // 2
    chunks = 3 * SLABS
    groups = pairs_y // 8
    units = groups * 4
    me_row = lax.axis_index("row")
    me_col = lax.axis_index("col")

    def where_of(k):
        return k // SLABS, k % SLABS

    barrier = pltpu.get_barrier_semaphore()
    for step in range(1, row_count):
        peer = lax.rem(me_row + step, row_count)
        pl.semaphore_signal(barrier, 1, device_id={"row": peer}, device_id_type=MESH)
    for step in range(1, col_count):
        peer = lax.rem(me_col + step, col_count)
        pl.semaphore_signal(barrier, 1, device_id={"col": peer}, device_id_type=MESH)

    def source_copy(k, slot):
        c, q = where_of(k)
        return pltpu.make_async_copy(
            krylov.at[blocks - 1, :, c, pl.ds(q * depth, depth)],
            source_slot.at[slot],
            source_sem.at[slot],
        )

    def chi_copy(k, slot):
        q = k % SLABS
        return pltpu.make_async_copy(
            chi.at[pl.ds(q * depth, depth)], chi_slot.at[slot], chi_sem.at[slot]
        )

    def image_copy(k, slot):
        c, q = where_of(k)
        return pltpu.make_async_copy(
            image_slot.at[slot],
            image.at[:, c, pl.ds(q * depth, depth)],
            image_sem.at[slot],
        )

    def green_copies(i, slot):
        entry = i % 6
        group = i // 6 % groups
        return [
            pltpu.make_async_copy(
                green.at[entry, :, pl.ds(half * pairs_y + group * 8, 8)],
                green_slot.at[slot, half],
                green_sem.at[slot, half],
            )
            for half in range(2)
        ]

    def send(axis, count, me, src, dst, send_sem, recv_sem, local_sem):
        for step in range(1, count):
            peer = lax.rem(me + step, count)
            pltpu.make_async_remote_copy(
                src_ref=src(peer),
                dst_ref=dst(me),
                send_sem=send_sem,
                recv_sem=recv_sem,
                device_id={axis: peer},
                device_id_type=MESH,
            ).start()
        pltpu.make_async_copy(src(me), dst(me), local_sem).start()

    def row_part(grid, h, k):
        c, q = where_of(k)
        return lambda p: grid.at[h, p, c, pl.ds(q * pair_depth, pair_depth)]

    def col_part(grid, h, k):
        c, q = where_of(k)
        return lambda j: grid.at[h, j, c, pl.ds(q * depth, depth)]

    def many(grid, h, k, count, size):
        c, q = where_of(k)
        return grid.at[h, pl.ds(0, count - 1), c, pl.ds(q * size, size)]

    def wait_bytes(ref, sem):
        pltpu.make_async_copy(ref, ref, sem).wait()

    def wait_row(grid, h, k, recv, local):
        n = h * chunks + k
        wait_bytes(many(grid, h, k, row_count, pair_depth), recv.at[n])
        wait_bytes(row_part(grid, h, k)(me_row), local.at[n])

    def wait_col(grid, h, k, recv, local):
        n = h * chunks + k
        wait_bytes(many(grid, h, k, col_count, depth), recv.at[n])
        wait_bytes(col_part(grid, h, k)(me_col), local.at[n])

    def send_row(src, dst, h, k, sems):
        n = h * chunks + k
        send("row", row_count, me_row, row_part(src, h, k), row_part(dst, h, k),
             sems[0].at[n], sems[1].at[n], sems[2].at[n])

    def send_col(src, dst, h, k, sems):
        n = h * chunks + k
        send("col", col_count, me_col, col_part(src, h, k), col_part(dst, h, k),
             sems[0].at[n], sems[1].at[n], sems[2].at[n])

    def ahead_lines(h, k, i):
        c, q = where_of(k)
        slot = i % 2
        source_copy(k, slot).wait()

        @pl.when(i + 1 < 2 * chunks)
        def _():
            source_copy((i + 1) % chunks, 1 - slot).start()

        rows = []
        for zb in range(2):
            members = [
                jnp.concatenate([source_slot[slot, r, 2 * z + zb] for z in range(pair_depth)], axis=0)
                for r in range(2)
            ]
            rows.append(jnp.concatenate(members, axis=1))
        result = right_product(jnp.concatenate(rows, axis=0), ahead_x[h])
        count = pair_depth * local_y
        for pp in range(row_count // 2):
            part = result[:, pp * LANES : (pp + 1) * LANES]
            first, second = swap_lanes(part[:count], part[count:])
            for b, value in ((0, first), (1, second)):
                grid_a[h, 2 * pp + b, c, pl.ds(q * pair_depth, pair_depth)] = value.reshape(
                    pair_depth, local_y, LANES
                )
        send_row(grid_a, grid_b, h, k, (f1s, f1r, f1l))

    def ahead_columns(h, k):
        c, q = where_of(k)
        wait_row(grid_b, h, k, f1r, f1l)

        def step(t, carry):
            z0 = q * pair_depth + 2 * t
            columns = [
                grid_b[h, :, c, z0 + i].reshape(row_count * local_y, LANES) for i in range(2)
            ]
            result = left_product(ahead_y[...], columns)
            for i in range(2):
                part = result[:, i * LANES : (i + 1) * LANES]
                part = part.reshape(col_count, 2, pairs_y, LANES)
                first, second = swap_lanes(part[:, 0], part[:, 1])
                grid_c[h, :, c, 2 * (z0 + i)] = first
                grid_c[h, :, c, 2 * (z0 + i) + 1] = second
            return carry

        lax.fori_loop(0, pair_depth // 2, step, 0)
        send_col(grid_c, grid_d, h, k, (f2s, f2r, f2l))

    def widen_green(h, group):
        for entry in range(6):
            i = (h * groups + group) * 6 + entry
            slot = entry % 2
            for copy in green_copies(i, slot):
                copy.wait()

            def step(t, carry):
                rows = pl.ds(t * 16, 16)
                wide = []
                for half in range(2):
                    value = green_slot[slot, half, rows].astype(jnp.float32)
                    value = value.reshape(16 * 8, 64)
                    wide.append(jnp.concatenate([value, value], axis=1))
                lane = lax.broadcasted_iota(jnp.int32, wide[0].shape, 1)
                value = jnp.where(
                    lane % 64 < 32,
                    pltpu.roll(wide[0], 96 * h, 1),
                    pltpu.roll(wide[1], 32 * (1 - h), 1),
                )
                green_wide[entry, pl.ds(t * 128, 128)] = value
                return carry

            lax.fori_loop(0, full_z // 16, step, 0)

            @pl.when(i + 2 < 2 * groups * 6)
            def _():
                for copy in green_copies(i + 2, slot):
                    copy.start()

    def mix(h, unit):
        group = unit // 4
        pair = unit % 4

        @pl.when(pair == 0)
        def _():
            widen_green(h, group)

        ky = group * 8 + pair * 2
        flat = [
            [grid_d.at[h, j, c].reshape(local_z * pairs_y, LANES) for c in range(3)]
            for j in range(col_count)
        ]
        for c in range(3):
            columns = []
            for i in range(2):
                pieces = [
                    flat[j][c][pl.ds(ky + i, local_z, stride=pairs_y), :] for j in range(col_count)
                ]
                columns.append(jnp.concatenate(pieces, axis=0))
            mixed[c] = left_product(ahead_z[...], columns)
        for c in range(3):
            columns = []
            for i in range(2):
                total = None
                for other in range(3):
                    weight = green_wide[
                        tensor_pairs[c][other], pl.ds(pair * 2 + i, full_z, stride=8), :
                    ]
                    term = weight * mixed[other, :, i * LANES : (i + 1) * LANES]
                    total = term if total is None else total + term
                columns.append(total)
            result = left_product(back_z[...], columns)
            for i in range(2):
                for j in range(col_count):
                    flat[j][c][pl.ds(ky + i, local_z, stride=pairs_y), :] = result[
                        j * local_z : (j + 1) * local_z, i * LANES : (i + 1) * LANES
                    ]

    def mix_some(h, k):
        def step(unit, carry):
            mix(h, unit)
            return carry

        lax.fori_loop(k * units // chunks, (k + 1) * units // chunks, step, 0)

    def back_columns(h, k):
        c, q = where_of(k)
        wait_col(grid_c, h, k, b1r, b1l)

        def step(t, carry):
            z0 = q * pair_depth + 2 * t
            columns = []
            for i in range(2):
                first, second = swap_lanes(
                    grid_c[h, :, c, 2 * (z0 + i)], grid_c[h, :, c, 2 * (z0 + i) + 1]
                )
                pieces = []
                for j in range(col_count):
                    pieces += [first[j], second[j]]
                columns.append(jnp.concatenate(pieces, axis=0))
            result = left_product(back_y[...], columns)
            for i in range(2):
                part = result[:, i * LANES : (i + 1) * LANES]
                grid_b[h, :, c, z0 + i] = part.reshape(row_count, local_y, LANES)
            return carry

        lax.fori_loop(0, pair_depth // 2, step, 0)
        send_row(grid_b, grid_a, h, k, (b2s, b2r, b2l))

    def back_lines(k):
        c, q = where_of(k)
        slot = k % 2
        for h in range(2):
            wait_row(grid_a, h, k, b2r, b2l)
        count = pair_depth * local_y
        low, high = [], []
        for h in range(2):
            for pp in range(row_count // 2):
                values = [
                    grid_a[h, 2 * pp + b, c, pl.ds(q * pair_depth, pair_depth)].reshape(count, LANES)
                    for b in range(2)
                ]
                first, second = swap_lanes(*values)
                low.append(first)
                high.append(second)
        rows = jnp.concatenate(
            [jnp.concatenate(low, axis=1), jnp.concatenate(high, axis=1)], axis=0
        )
        result = right_product(rows, back_x[...])
        source_copy(k, slot).wait()
        chi_copy(k, slot).wait()

        @pl.when(k >= 2)
        def _():
            image_copy(k - 2, slot).wait()

        for zb in range(2):
            for z in range(pair_depth):
                start = zb * count + z * local_y
                for r in range(2):
                    image_slot[slot, r, 2 * z + zb] = (
                        source_slot[slot, r, 2 * z + zb]
                        - chi_slot[slot, 2 * z + zb]
                        * result[start : start + local_y, r * half_x : (r + 1) * half_x]
                    )
        image_copy(k, slot).start()

        @pl.when(k + 2 < chunks)
        def _():
            source_copy(k + 2, slot).start()
            chi_copy(k + 2, slot).start()

    def loop(body):
        def step(k, carry):
            body(k)
            return carry

        lax.fori_loop(0, chunks, step, 0)

    source_copy(0, 0).start()
    for i in range(2):
        for copy in green_copies(i, i):
            copy.start()
    pl.semaphore_wait(barrier, row_count + col_count - 2)

    loop(lambda k: ahead_lines(0, k, k))

    def stage_one(k):
        ahead_columns(0, k)
        ahead_lines(1, k, k + chunks)

    loop(stage_one)

    def free_rows(k):
        for h in range(2):
            wait_bytes(many(grid_a, h, k, row_count, pair_depth), f1s.at[h * chunks + k])

    def free_cols(h):
        loop(
            lambda k: wait_bytes(
                many(grid_c, h, k, col_count, depth), f2s.at[h * chunks + k]
            )
        )
        for step in range(1, col_count):
            peer = lax.rem(me_col + step, col_count)
            pl.semaphore_signal(
                col_credit.at[h], 1, device_id={"col": peer}, device_id_type=MESH
            )

    loop(lambda k: wait_col(grid_d, 0, k, f2r, f2l))

    def stage_two(k):
        ahead_columns(1, k)
        mix_some(0, k)

    loop(stage_two)
    free_cols(0)
    pl.semaphore_wait(col_credit.at[0], col_count - 1)
    loop(lambda k: send_col(grid_d, grid_c, 0, k, (b1s, b1r, b1l)))
    loop(free_rows)
    for step in range(1, row_count):
        peer = lax.rem(me_row + step, row_count)
        pl.semaphore_signal(row_credit, 1, device_id={"row": peer}, device_id_type=MESH)
    loop(lambda k: wait_col(grid_d, 1, k, f2r, f2l))
    pl.semaphore_wait(row_credit, row_count - 1)

    def stage_three(k):
        mix_some(1, k)
        back_columns(0, k)

    loop(stage_three)
    free_cols(1)
    pl.semaphore_wait(col_credit.at[1], col_count - 1)
    loop(lambda k: send_col(grid_d, grid_c, 1, k, (b1s, b1r, b1l)))
    for k in range(2):
        source_copy(k, k).start()
        chi_copy(k, k).start()

    def stage_four(k):
        back_columns(1, k)

        @pl.when(k >= 1)
        def _():
            back_lines(k - 1)

    loop(stage_four)
    back_lines(jnp.int32(chunks - 1))
    for k in range(chunks - 2, chunks):
        image_copy(k, k % 2).wait()

    def finish(k):
        for h in range(2):
            n = h * chunks + k
            wait_bytes(many(grid_d, h, k, col_count, depth), b1s.at[n])
            wait_bytes(many(grid_b, h, k, row_count, pair_depth), b2s.at[n])

    loop(finish)


def fits_kernel(susceptibility, green_spectra):
    local_z, local_y, half_x = susceptibility.shape
    full_z, part_y, part_x = green_spectra.shape[1:]
    return (
        part_x == LANES // 2
        and part_y % 16 == 0
        and full_z % 16 == 0
        and local_y % 8 == 0
        and local_z % (4 * SLABS) == 0
        and half_x % LANES == 0
        and lax.axis_size("row") % 2 == 0
    )


def field_image(krylov_basis, susceptibility, green_spectra):
    row_count = lax.axis_size("row")
    col_count = lax.axis_size("col")
    local_z, local_y, half_x = susceptibility.shape
    full_z, part_y, part_x = green_spectra.shape[1:]
    scaling = 1.0 / (4.0 * half_x * full_z * local_y * row_count)
    ahead_x, back_x = line_tables(half_x, row_count, part_x, scaling)
    ahead_y, back_y = left_tables(local_y * row_count)
    ahead_z, back_z = left_tables(local_z * col_count)
    depth = local_z // SLABS
    pairs_y = part_y // 2
    row_grid = pltpu.VMEM((2, row_count, 3, local_z // 2, local_y, LANES), jnp.float32)
    col_grid = pltpu.VMEM((2, col_count, 3, local_z, pairs_y, LANES), jnp.float32)
    dma = pltpu.SemaphoreType.DMA
    whole = pl.BlockSpec(memory_space=pltpu.VMEM)
    outside = pl.BlockSpec(memory_space=pl.ANY)
    return pl.pallas_call(
        functools.partial(field_kernel, row_count, col_count),
        out_shape=jax.ShapeDtypeStruct((2, 3, local_z, local_y, half_x), jnp.float32),
        in_specs=[outside] * 3 + [whole] * 6,
        out_specs=outside,
        scratch_shapes=[
            row_grid,
            row_grid,
            col_grid,
            col_grid,
            pltpu.VMEM((2, 2, full_z, 8, part_x), jnp.bfloat16),
            pltpu.VMEM((6, full_z * 8, LANES), jnp.float32),
            pltpu.VMEM((2, 2, depth, local_y, half_x), jnp.float32),
            pltpu.VMEM((2, depth, local_y, half_x), jnp.float32),
            pltpu.VMEM((2, 2, depth, local_y, half_x), jnp.float32),
            pltpu.VMEM((3, full_z, 2 * LANES), jnp.float32),
        ]
        + [dma((2 * 3 * SLABS,))] * 12
        + [
            dma((2, 2)),
            dma((2,)),
            dma((2,)),
            dma((2,)),
            pltpu.SemaphoreType.REGULAR,
            pltpu.SemaphoreType.REGULAR((2,)),
        ],
        compiler_params=pltpu.CompilerParams(
            collective_id=0, has_side_effects=True, vmem_limit_bytes=67043328
        ),
        name="field_image",
    )(krylov_basis, susceptibility, green_spectra, ahead_x, back_x, ahead_y, back_y, ahead_z, back_z)


def total_over_devices(partial):
    return jnp.sum(lax.all_gather(partial, ("row", "col")), axis=0)


def per_device(krylov_basis, susceptibility, green_spectra):
    blocks = krylov_basis.shape[0]
    latest = krylov_basis[-1]
    if fits_kernel(susceptibility, green_spectra):
        image = field_image(krylov_basis, susceptibility, green_spectra)
    else:
        response = convolve(latest, green_spectra)
        image = [latest[:, c] - susceptibility[None] * response[c] for c in range(3)]
        image = jnp.stack(image, axis=1)
    entry_count = 3.0 * susceptibility.size * lax.axis_size("row") * lax.axis_size("col")
    basis = krylov_basis.reshape((2 * blocks,) + image.shape[1:])
    local_coeffs = jnp.stack(
        [jnp.sum(basis * image[j][None], axis=(1, 2, 3, 4)) for j in range(2)], axis=1
    )
    coefficients = total_over_devices(local_coeffs / entry_count)
    projected = []
    for j in range(2):
        column = image[j]
        for a in range(2 * blocks):
            column = column - coefficients[a, j] * basis[a]
        projected.append(column)
    g00 = jnp.sum(projected[0] * projected[0])
    g01 = jnp.sum(projected[0] * projected[1])
    g11 = jnp.sum(projected[1] * projected[1])
    gram = total_over_devices(jnp.stack([g00, g01, g11]) / entry_count)
    lead_norm = jnp.sqrt(gram[0] + 1e-06)
    cross_term = gram[1] / lead_norm
    tail_norm = jnp.sqrt(gram[2] - cross_term * cross_term + 1e-06)
    first_column = projected[0] / lead_norm
    second_column = (projected[1] - cross_term * first_column) / tail_norm
    next_block = jnp.stack([first_column, second_column])
    block_factor = jnp.stack(
        [jnp.stack([lead_norm, cross_term]), jnp.stack([jnp.zeros_like(lead_norm), tail_norm])]
    )
    return (coefficients.reshape(blocks, 2, 2), next_block, block_factor)


def solution(mesh):
    in_specs = (
        P(None, None, None, "col", "row", None),
        P("col", "row", None),
        P(None, None, "col", "row"),
    )
    out_specs = (P(), P(None, None, "col", "row", None), P())
    return jax.shard_map(
        per_device, mesh=mesh, in_specs=in_specs, out_specs=out_specs, check_vma=False
    )
```

```python
import functools
import math

import jax
import jax.numpy as jnp
from jax import lax
from jax.experimental import pallas as pl
from jax.experimental.pallas import tpu as pltpu
from jax.sharding import PartitionSpec as P

fast = lax.Precision.HIGH
tensor_pairs = ((0, 3, 4), (3, 1, 5), (4, 5, 2))


def twiddle(count_in, count_out, period, orient, factor):
    row_index = lax.broadcasted_iota(jnp.int32, (count_in, count_out), 0)
    col_index = lax.broadcasted_iota(jnp.int32, (count_in, count_out), 1)
    phases = row_index * col_index % period
    angles = phases.astype(jnp.float32) * (2.0 * math.pi / period)
    cosine = jnp.cos(angles) * factor
    sines = jnp.sin(angles) * (orient * factor)
    return jnp.stack([jnp.stack([cosine, sines]), jnp.stack([-sines, cosine])])


def exchange_rows(blocks):
    return lax.all_to_all(blocks, "row", split_axis=0, concat_axis=0, tiled=True)


def exchange_cols(blocks):
    return lax.all_to_all(blocks, "col", split_axis=0, concat_axis=0, tiled=True)


def forward(source, table_x, table_y, table_z):
    local_z, local_y = source.shape[1:3]
    row_count, part_x = table_x.shape[-2:]
    col_count, part_y = table_y.shape[-2:]
    spectra = jnp.einsum("rzyx,rsxdl->dsyzl", source, table_x, precision=fast)
    spectra = spectra.reshape(row_count, 2, local_y, local_z * part_x)
    spectra = exchange_rows(spectra)
    spectra = spectra.transpose(1, 0, 2, 3).reshape(2, row_count * local_y, local_z, part_x)
    spectra = jnp.einsum("ryzl,rsyeq->eszql", spectra, table_y, precision=fast)
    spectra = spectra.reshape(col_count, 2, local_z, part_y * part_x)
    spectra = exchange_cols(spectra)
    spectra = spectra.transpose(1, 0, 2, 3).reshape(2, col_count * local_z, part_y * part_x)
    return jnp.einsum("rzb,rszk->skb", spectra, table_z, precision=fast)


def backward(spectra, back_x, back_y, back_z):
    row_count, part_x = back_x.shape[2:4]
    col_count, part_y, width = back_y.shape[2:]
    spectra = jnp.einsum("rkb,rskz->szb", spectra, back_z, precision=fast)
    local_z = spectra.shape[1] // col_count
    spectra = spectra.reshape(2, col_count, local_z, part_y * part_x).transpose(1, 0, 2, 3)
    spectra = exchange_cols(spectra)
    spectra = spectra.reshape(col_count, 2, local_z, part_y, part_x)
    spectra = jnp.einsum("erzql,rseqy->syzl", spectra, back_y, precision=fast)
    local_y = width // row_count
    spectra = spectra.reshape(2, row_count, local_y, local_z * part_x).transpose(1, 0, 2, 3)
    spectra = exchange_rows(spectra)
    spectra = spectra.reshape(row_count, 2, local_y, local_z, part_x)
    return jnp.einsum("dryzl,rsdlx->szyx", spectra, back_x, precision=fast)


def convolve(source, green_spectra):
    row_count = lax.axis_size("row")
    col_count = lax.axis_size("col")
    width_x = 2 * source.shape[-1]
    width_y = 2 * source.shape[-2] * row_count
    width_z = 2 * source.shape[-3] * col_count
    part_x = width_x // row_count
    part_y = width_y // col_count
    half_x, half_y, half_z = width_x // 2, width_y // 2, width_z // 2
    table_x = twiddle(half_x, width_x, width_x, -1.0, 1.0).reshape(2, 2, half_x, row_count, part_x)
    table_y = twiddle(half_y, width_y, width_y, -1.0, 1.0).reshape(2, 2, half_y, col_count, part_y)
    table_z = twiddle(half_z, width_z, width_z, -1.0, 1.0)
    spectra = [forward(source[:, c], table_x, table_y, table_z) for c in range(3)]
    coupling = green_spectra.astype(jnp.float32).reshape(6, width_z, part_y * part_x)
    back_z = twiddle(width_z, half_z, width_z, 1.0, 1.0)
    back_y = twiddle(width_y, half_y, width_y, 1.0, 1.0).reshape(2, 2, col_count, part_y, half_y)
    scaling = 1.0 / (width_x * width_y * width_z)
    back_x = twiddle(width_x, half_x, width_x, 1.0, scaling).reshape(2, 2, row_count, part_x, half_x)
    result = []
    for member in range(3):
        chosen = tensor_pairs[member]
        total = coupling[chosen[0]] * spectra[0]
        total = total + coupling[chosen[1]] * spectra[1]
        total = total + coupling[chosen[2]] * spectra[2]
        result.append(backward(total, back_x, back_y, back_z))
    return result


LANES = 128
SLABS = 4
MESH = pl.DeviceIdType.MESH


def cosine_of(phase, period):
    quarter = period // 4
    turn = (phase + quarter // 2) // quarter
    angle = (phase - turn * quarter).astype(jnp.float32) * (2.0 * math.pi / period)
    square = angle * angle
    even = 1.0 / 24 - square * (1.0 / 720 - square * (1.0 / 40320))
    even = 1.0 - square * (0.5 - square * even)
    odd = 1.0 / 120 - square * (1.0 / 5040 - square * (1.0 / 362880))
    odd = angle * (1.0 - square * (1.0 / 6 - square * odd))
    value = jnp.where(turn % 2 == 0, even, odd)
    return jnp.where((turn + 1) % 4 < 2, value, -value)


def halves(value):
    high = value.astype(jnp.bfloat16)
    return high, (value - high.astype(jnp.float32)).astype(jnp.bfloat16)


def iota(shape, axis):
    return lax.broadcasted_iota(jnp.int32, shape, axis)


def swap_lanes(first, second):
    last = first.ndim - 1
    lane = lax.broadcasted_iota(jnp.int32, first.shape, last)
    keep = lane % 64 < 32
    return (
        jnp.where(keep, first, pltpu.roll(second, 32, last)),
        jnp.where(keep, pltpu.roll(first, 96, last), second),
    )


def stacked_operand(column):
    sign = jnp.where(iota(column.shape, 1) < 64, 1.0, -1.0)
    high, low = halves(jnp.concatenate([column, pltpu.roll(column, 64, 1) * sign], axis=0))
    return jnp.concatenate([high, low, high], axis=0)


def left_product(table, columns):
    operand = jnp.concatenate([stacked_operand(column) for column in columns], axis=1)
    return jnp.dot(table, operand, preferred_element_type=jnp.float32)


def right_product(rows, table_high, table_low, flip):
    dims = (((1,), (1,) if flip else (0,)), ((), ()))
    high, low = halves(rows)
    both = jnp.concatenate([high, low], axis=0)
    main = lax.dot_general(both, table_high, dims, preferred_element_type=jnp.float32)
    rest = lax.dot_general(high, table_low, dims, preferred_element_type=jnp.float32)
    count = rows.shape[0]
    return main[:count] + (main[count:] + rest)


def field_kernel(
    row_count,
    col_count,
    krylov,
    chi,
    green,
    next_block,
    coefficients,
    factor,
    grid_a,
    grid_b,
    grid_c,
    grid_d,
    line_table,
    ahead_table,
    back_table,
    basis,
    chi_all,
    image,
    green_slot,
    weights,
    mixed,
    sums,
    gather_one,
    gather_two,
    f1s, f1r, f1l, f2s, f2r, f2l, b1s, b1r, b1l, b2s, b2r, b2l,
    green_sem,
    basis_sem,
    source_sem,
    chi_sem,
    out_sem,
    gather_send,
    gather_recv,
    row_credit,
    col_credit,
):
    blocks = krylov.shape[0]
    local_z, local_y, half_x = chi.shape
    pairs_y = grid_c.shape[4]
    full_z = green.shape[3]
    half_y = local_y * row_count
    part_x = green.shape[2]
    world = row_count * col_count
    depth = local_z // SLABS
    pair_depth = depth // 2
    chunks = 3 * SLABS
    units = pairs_y // 2
    me_row = lax.axis_index("row")
    me_col = lax.axis_index("col")

    def where_of(k):
        return k // SLABS, k % SLABS

    barrier = pltpu.get_barrier_semaphore()
    me = me_row * col_count + me_col

    def others(body):
        for i in range(row_count):
            for j in range(col_count):
                if i or j:
                    peer_row = lax.rem(me_row + i, row_count)
                    peer_col = lax.rem(me_col + j, col_count)
                    body({"row": peer_row, "col": peer_col})

    others(lambda peer: pl.semaphore_signal(barrier, 1, device_id=peer, device_id_type=MESH))

    source = basis.at[blocks - 1]

    def source_copy(c):
        return pltpu.make_async_copy(krylov.at[blocks - 1, :, c], source.at[:, c], source_sem.at[c])

    older = pltpu.make_async_copy(
        krylov.at[pl.ds(0, blocks - 1)], basis.at[pl.ds(0, blocks - 1)], basis_sem
    )
    chi_copy = pltpu.make_async_copy(chi, chi_all, chi_sem)

    def out_copy(c):
        return pltpu.make_async_copy(image.at[:, c], next_block.at[:, c], out_sem.at[c])

    def green_copies(i):
        slot = i % 2
        h = i // units
        pair = i % units * 2
        return [
            pltpu.make_async_copy(
                green.at[:, pl.ds(half * pairs_y + pair, 2), pl.ds(h * 32, 32)],
                green_slot.at[slot, half],
                green_sem.at[slot, half],
            )
            for half in range(2)
        ]

    def build_line_table():
        rows = 64
        for h in range(2):

            def step(t, carry):
                shape = (rows, row_count * part_x)
                row = iota(shape, 0) + t * rows
                col = iota(shape, 1)
                point = row % half_x
                freq = col // LANES * (2 * part_x) + col // 32 % 2 * part_x + h * 32 + col % 32
                turn = col // 64 % 2 - row // half_x
                phase = (point * freq + (turn + 4) * (half_x // 2)) % (2 * half_x)
                high, low = halves(cosine_of(phase, 2 * half_x))
                line_table[h, 0, pl.ds(t * rows, rows)] = high
                line_table[h, 1, pl.ds(t * rows, rows)] = low
                return carry

            lax.fori_loop(0, 2 * half_x // rows, step, 0)

    def build_left_tables():
        rows = 64

        def step(t, carry):
            shape = (rows, 2 * half_y)
            freq = iota(shape, 0) + t * rows
            col = iota(shape, 1)
            phase = freq * (col % half_y) + (4 - col // half_y) * (half_y // 2)
            high, low = halves(cosine_of(phase % (2 * half_y), 2 * half_y))
            ahead_table[pl.ds(t * rows, rows)] = jnp.concatenate([high, high, low], axis=1)
            return carry

        lax.fori_loop(0, 2 * half_y // rows, step, 0)

        def back_step(t, carry):
            shape = (rows, 4 * half_y)
            point = iota(shape, 0) + t * rows
            col = iota(shape, 1)
            phase = point * (col % (2 * half_y)) + col // (2 * half_y) * (half_y // 2)
            high, low = halves(cosine_of(phase % (2 * half_y), 2 * half_y))
            back_table[pl.ds(t * rows, rows)] = jnp.concatenate([high, high, low], axis=1)
            return carry

        lax.fori_loop(0, half_y // rows, back_step, 0)

    def send(axis, count, me, src, dst, send_sem, recv_sem, local_sem):
        for step in range(1, count):
            peer = lax.rem(me + step, count)
            pltpu.make_async_remote_copy(
                src_ref=src(peer),
                dst_ref=dst(me),
                send_sem=send_sem,
                recv_sem=recv_sem,
                device_id={axis: peer},
                device_id_type=MESH,
            ).start()
        pltpu.make_async_copy(src(me), dst(me), local_sem).start()

    def row_part(grid, h, k):
        c, q = where_of(k)
        return lambda p: grid.at[h, p, c, pl.ds(q * pair_depth, pair_depth)]

    def col_part(grid, h, k):
        c, q = where_of(k)
        return lambda j: grid.at[h, j, c, pl.ds(q * depth, depth)]

    def many(grid, h, k, count, size):
        c, q = where_of(k)
        return grid.at[h, pl.ds(0, count - 1), c, pl.ds(q * size, size)]

    def wait_bytes(ref, sem):
        pltpu.make_async_copy(ref, ref, sem).wait()

    def wait_row(grid, h, k, recv, local):
        n = h * chunks + k
        wait_bytes(many(grid, h, k, row_count, pair_depth), recv.at[n])
        wait_bytes(row_part(grid, h, k)(me_row), local.at[n])

    def wait_col(grid, h, k, recv, local):
        n = h * chunks + k
        wait_bytes(many(grid, h, k, col_count, depth), recv.at[n])
        wait_bytes(col_part(grid, h, k)(me_col), local.at[n])

    def send_row(src, dst, h, k, sems):
        n = h * chunks + k
        send("row", row_count, me_row, row_part(src, h, k), row_part(dst, h, k),
             sems[0].at[n], sems[1].at[n], sems[2].at[n])

    def send_col(src, dst, h, k, sems):
        n = h * chunks + k
        send("col", col_count, me_col, col_part(src, h, k), col_part(dst, h, k),
             sems[0].at[n], sems[1].at[n], sems[2].at[n])

    def ahead_lines(h, k):
        c, q = where_of(k)
        rows = []
        for zb in range(2):
            members = [
                jnp.concatenate(
                    [source[r, c, q * depth + 2 * z + zb] for z in range(pair_depth)], axis=0
                )
                for r in range(2)
            ]
            rows.append(jnp.concatenate(members, axis=1))
        result = right_product(
            jnp.concatenate(rows, axis=0), line_table[h, 0], line_table[h, 1], False
        )
        count = pair_depth * local_y
        for pp in range(row_count // 2):
            part = result[:, pp * LANES : (pp + 1) * LANES]
            first, second = swap_lanes(part[:count], part[count:])
            for b, value in ((0, first), (1, second)):
                grid_a[h, 2 * pp + b, c, pl.ds(q * pair_depth, pair_depth)] = value.reshape(
                    pair_depth, local_y, LANES
                )
        send_row(grid_a, grid_b, h, k, (f1s, f1r, f1l))

    def ahead_columns(h, k):
        c, q = where_of(k)
        wait_row(grid_b, h, k, f1r, f1l)

        def step(t, carry):
            z0 = q * pair_depth + 2 * t
            columns = [
                grid_b[h, :, c, z0 + i].reshape(row_count * local_y, LANES) for i in range(2)
            ]
            result = left_product(ahead_table[...], columns)
            for i in range(2):
                part = result[:, i * LANES : (i + 1) * LANES]
                part = part.reshape(col_count, 2, pairs_y, LANES)
                first, second = swap_lanes(part[:, 0], part[:, 1])
                grid_c[h, :, c, 2 * (z0 + i)] = first
                grid_c[h, :, c, 2 * (z0 + i) + 1] = second
            return carry

        lax.fori_loop(0, pair_depth // 2, step, 0)
        send_col(grid_c, grid_d, h, k, (f2s, f2r, f2l))

    def mix(h, unit):
        step = h * units + unit
        slot = step % 2
        ky = unit * 2
        flat = [
            [grid_d.at[h, j, c].reshape(local_z * pairs_y, LANES) for c in range(3)]
            for j in range(col_count)
        ]
        for c in range(3):
            columns = []
            for i in range(2):
                pieces = [
                    flat[j][c][pl.ds(ky + i, local_z, stride=pairs_y), :] for j in range(col_count)
                ]
                columns.append(jnp.concatenate(pieces, axis=0))
            mixed[c] = left_product(ahead_table[...], columns)
        for copy in green_copies(step):
            copy.wait()
        for entry in range(6):
            for i in range(2):
                first = green_slot[slot, 0, entry, i]
                second = green_slot[slot, 1, entry, i]
                block = jnp.concatenate([first, second, first, second], axis=0)
                weights[entry, :, i * LANES : (i + 1) * LANES] = block.T.astype(jnp.float32)

        @pl.when(step + 2 < 2 * units)
        def _():
            for copy in green_copies(step + 2):
                copy.start()

        for c in range(3):
            columns = []
            for i in range(2):
                part = slice(i * LANES, (i + 1) * LANES)
                total = None
                for other in range(3):
                    term = weights[tensor_pairs[c][other], :, part] * mixed[other, :, part]
                    total = term if total is None else total + term
                columns.append(total)
            result = left_product(back_table[...], columns)
            for i in range(2):
                for j in range(col_count):
                    flat[j][c][pl.ds(ky + i, local_z, stride=pairs_y), :] = result[
                        j * local_z : (j + 1) * local_z, i * LANES : (i + 1) * LANES
                    ]

    def mix_some(h, k):
        def step(unit, carry):
            mix(h, unit)
            return carry

        lax.fori_loop(k * units // chunks, (k + 1) * units // chunks, step, 0)

    def back_columns(h, k):
        c, q = where_of(k)
        wait_col(grid_c, h, k, b1r, b1l)

        def step(t, carry):
            z0 = q * pair_depth + 2 * t
            columns = []
            for i in range(2):
                first, second = swap_lanes(
                    grid_c[h, :, c, 2 * (z0 + i)], grid_c[h, :, c, 2 * (z0 + i) + 1]
                )
                pieces = []
                for j in range(col_count):
                    pieces += [first[j], second[j]]
                columns.append(jnp.concatenate(pieces, axis=0))
            result = left_product(back_table[...], columns)
            for i in range(2):
                part = result[:, i * LANES : (i + 1) * LANES]
                grid_b[h, :, c, z0 + i] = part.reshape(row_count, local_y, LANES)
            return carry

        lax.fori_loop(0, pair_depth // 2, step, 0)
        send_row(grid_b, grid_a, h, k, (b2s, b2r, b2l))

    scaling = 1.0 / (4.0 * half_x * half_y * full_z)

    def back_lines(k):
        c, q = where_of(k)
        for h in range(2):
            wait_row(grid_a, h, k, b2r, b2l)
        count = pair_depth * local_y
        result = None
        for h in range(2):
            low, high = [], []
            for pp in range(row_count // 2):
                values = [
                    grid_a[h, 2 * pp + b, c, pl.ds(q * pair_depth, pair_depth)].reshape(count, LANES)
                    for b in range(2)
                ]
                first, second = swap_lanes(*values)
                low.append(first)
                high.append(second)
            rows = jnp.concatenate(
                [jnp.concatenate(low, axis=1), jnp.concatenate(high, axis=1)], axis=0
            )
            term = right_product(rows, line_table[h, 0], line_table[h, 1], True)
            result = term if result is None else result + term
        partial = [None] * (4 * blocks)
        for zb in range(2):
            for pair in range(pair_depth):
                z = q * depth + 2 * pair + zb
                start = zb * count + pair * local_y
                weight = chi_all[z] * scaling
                columns = []
                for r in range(2):
                    value = (
                        source[r, c, z]
                        - weight * result[start : start + local_y, r * half_x : (r + 1) * half_x]
                    )
                    image[r, c, z] = value
                    columns.append(value)
                for a in range(2 * blocks):
                    member = basis[a // 2, a % 2, c, z]
                    for r in range(2):
                        term = fold(member * columns[r])
                        old = partial[2 * a + r]
                        partial[2 * a + r] = term if old is None else old + term
        for i in range(4 * blocks):
            sums[i] = sums[i] + partial[i]

    def exchange(gather, n):
        def start(peer):
            pltpu.make_async_remote_copy(
                src_ref=gather.at[me],
                dst_ref=gather.at[me],
                send_sem=gather_send.at[n],
                recv_sem=gather_recv.at[n],
                device_id=peer,
                device_id_type=MESH,
            ).start()

        others(start)
        rest = gather.at[pl.ds(0, world - 1)]
        wait_bytes(rest, gather_recv.at[n])
        wait_bytes(rest, gather_send.at[n])
        total = gather[0]
        for i in range(1, world):
            total = total + gather[i]
        return jnp.sum(total, axis=1, keepdims=True) * (1.0 / (3.0 * chi_all.size * world))

    def orthonormalize():
        gather_one[me] = jnp.sum(sums[...], axis=1)
        products = exchange(gather_one, 0)
        coefficients[...] = jnp.broadcast_to(products, coefficients.shape)
        zero = jnp.zeros((8, LANES), jnp.float32)

        def project(z, totals):
            totals = list(totals)
            for c in range(3):
                columns = [image[r, c, z] for r in range(2)]
                for a in range(2 * blocks):
                    member = basis[a // 2, a % 2, c, z]
                    for r in range(2):
                        i = 2 * a + r
                        columns[r] = columns[r] - products[i : i + 1] * member
                for r in range(2):
                    image[r, c, z] = columns[r]
                for n, (i, j) in enumerate(((0, 0), (0, 1), (1, 1))):
                    totals[n] = totals[n] + fold(columns[i] * columns[j])
            return tuple(totals)

        totals = lax.fori_loop(0, local_z, project, (zero, zero, zero))
        rows = [jnp.sum(total, axis=0, keepdims=True) for total in totals]
        gather_two[me] = jnp.concatenate(rows + [zero[:5]], axis=0)
        gram = exchange(gather_two, 1)
        lead = jnp.sqrt(gram[0:1] + 1e-06)
        cross = gram[1:2] / lead
        tail = jnp.sqrt(gram[2:3] - cross * cross + 1e-06)
        values = jnp.concatenate([lead, cross, zero[:1, :1], tail, zero[:4, :1]], axis=0)
        factor[...] = jnp.broadcast_to(values, factor.shape)
        lead_inverse = 1.0 / lead
        tail_inverse = 1.0 / tail
        for c in range(3):

            def scale(z, carry):
                first = image[0, c, z] * lead_inverse
                image[0, c, z] = first
                image[1, c, z] = (image[1, c, z] - cross * first) * tail_inverse
                return carry

            lax.fori_loop(0, local_z, scale, 0)
            out_copy(c).start()
        for c in range(3):
            out_copy(c).wait()

    def fold(value):
        total = None
        for i in range(local_y // 8):
            for j in range(half_x // LANES):
                piece = value[i * 8 : (i + 1) * 8, j * LANES : (j + 1) * LANES]
                total = piece if total is None else total + piece
        return total

    def loop(body):
        def step(k, carry):
            body(k)
            return carry

        lax.fori_loop(0, chunks, step, 0)

    for c in range(3):
        source_copy(c).start()
    for i in range(2):
        for copy in green_copies(i):
            copy.start()
    chi_copy.start()
    older.start()
    build_line_table()
    sums[...] = jnp.zeros(sums.shape, jnp.float32)
    for c in range(3):
        source_copy(c).wait()
    pl.semaphore_wait(barrier, world - 1)
    loop(lambda k: ahead_lines(0, k))
    build_left_tables()

    def stage_one(k):
        ahead_columns(0, k)
        ahead_lines(1, k)

    loop(stage_one)

    def free_rows(k):
        for h in range(2):
            wait_bytes(many(grid_a, h, k, row_count, pair_depth), f1s.at[h * chunks + k])

    def free_cols(h):
        loop(
            lambda k: wait_bytes(
                many(grid_c, h, k, col_count, depth), f2s.at[h * chunks + k]
            )
        )
        for step in range(1, col_count):
            peer = lax.rem(me_col + step, col_count)
            pl.semaphore_signal(
                col_credit.at[h], 1, device_id={"col": peer}, device_id_type=MESH
            )

    loop(lambda k: wait_col(grid_d, 0, k, f2r, f2l))

    def stage_two(k):
        ahead_columns(1, k)
        mix_some(0, k)

    loop(stage_two)
    free_cols(0)
    pl.semaphore_wait(col_credit.at[0], col_count - 1)
    loop(lambda k: send_col(grid_d, grid_c, 0, k, (b1s, b1r, b1l)))
    loop(free_rows)
    for step in range(1, row_count):
        peer = lax.rem(me_row + step, row_count)
        pl.semaphore_signal(row_credit, 1, device_id={"row": peer}, device_id_type=MESH)
    loop(lambda k: wait_col(grid_d, 1, k, f2r, f2l))
    pl.semaphore_wait(row_credit, row_count - 1)

    def stage_three(k):
        mix_some(1, k)
        back_columns(0, k)

    loop(stage_three)
    free_cols(1)
    pl.semaphore_wait(col_credit.at[1], col_count - 1)
    loop(lambda k: send_col(grid_d, grid_c, 1, k, (b1s, b1r, b1l)))
    chi_copy.wait()
    older.wait()

    def stage_four(k):
        back_columns(1, k)

        @pl.when(k >= 1)
        def _():
            back_lines(k - 1)

    loop(stage_four)
    back_lines(jnp.int32(chunks - 1))
    orthonormalize()

    def finish(k):
        for h in range(2):
            n = h * chunks + k
            wait_bytes(many(grid_d, h, k, col_count, depth), b1s.at[n])
            wait_bytes(many(grid_b, h, k, row_count, pair_depth), b2s.at[n])

    loop(finish)


def fits_kernel(susceptibility, green_spectra):
    local_z, local_y, half_x = susceptibility.shape
    full_z, part_y, part_x = green_spectra.shape[1:]
    return (
        part_x == LANES // 2
        and part_y % 16 == 0
        and full_z % LANES == 0
        and full_z == 2 * local_y * lax.axis_size("row")
        and local_y % 8 == 0
        and local_z % (4 * SLABS) == 0
        and half_x % LANES == 0
        and lax.axis_size("row") % 2 == 0
    )


def fused_step(krylov_basis, susceptibility, green_spectra):
    row_count = lax.axis_size("row")
    col_count = lax.axis_size("col")
    world = row_count * col_count
    blocks = krylov_basis.shape[0]
    local_z, local_y, half_x = susceptibility.shape
    full_z, part_y, part_x = green_spectra.shape[1:]
    half_y = local_y * row_count
    pairs_y = part_y // 2
    row_grid = pltpu.VMEM((2, row_count, 3, local_z // 2, local_y, LANES), jnp.float32)
    col_grid = pltpu.VMEM((2, col_count, 3, local_z, pairs_y, LANES), jnp.float32)
    dma = pltpu.SemaphoreType.DMA
    whole = pl.BlockSpec(memory_space=pltpu.VMEM)
    outside = pl.BlockSpec(memory_space=pl.ANY)
    field = (2, 3, local_z, local_y, half_x)
    next_block, coefficients, factor = pl.pallas_call(
        functools.partial(field_kernel, row_count, col_count),
        out_shape=(
            jax.ShapeDtypeStruct(field, jnp.float32),
            jax.ShapeDtypeStruct((4 * blocks, LANES), jnp.float32),
            jax.ShapeDtypeStruct((8, LANES), jnp.float32),
        ),
        in_specs=[outside] * 3,
        out_specs=(outside, whole, whole),
        scratch_shapes=[
            row_grid,
            row_grid,
            col_grid,
            col_grid,
            pltpu.VMEM((2, 2, 2 * half_x, row_count * part_x), jnp.bfloat16),
            pltpu.VMEM((2 * half_y, 6 * half_y), jnp.bfloat16),
            pltpu.VMEM((half_y, 12 * half_y), jnp.bfloat16),
            pltpu.VMEM((blocks,) + field, jnp.float32),
            pltpu.VMEM((local_z, local_y, half_x), jnp.float32),
            pltpu.VMEM(field, jnp.float32),
            pltpu.VMEM((2, 2, 6, 2, 32, full_z), jnp.bfloat16),
            pltpu.VMEM((6, full_z, 2 * LANES), jnp.float32),
            pltpu.VMEM((3, full_z, 2 * LANES), jnp.float32),
            pltpu.VMEM((4 * blocks, 8, LANES), jnp.float32),
            pltpu.VMEM((world, 4 * blocks, LANES), jnp.float32),
            pltpu.VMEM((world, 8, LANES), jnp.float32),
        ]
        + [dma((2 * 3 * SLABS,))] * 12
        + [
            dma((2, 2)),
            dma,
            dma((3,)),
            dma,
            dma((3,)),
            dma((2,)),
            dma((2,)),
            pltpu.SemaphoreType.REGULAR,
            pltpu.SemaphoreType.REGULAR((2,)),
        ],
        compiler_params=pltpu.CompilerParams(
            collective_id=0, has_side_effects=True, vmem_limit_bytes=67043328
        ),
        name="fused_step",
    )(krylov_basis, susceptibility, green_spectra.transpose(0, 2, 3, 1))
    projections = coefficients[:, 0].reshape(blocks, 2, 2)
    return projections, next_block, factor[:4, 0].reshape(2, 2)


def total_over_devices(partial):
    return jnp.sum(lax.all_gather(partial, ("row", "col")), axis=0)


def per_device(krylov_basis, susceptibility, green_spectra):
    blocks = krylov_basis.shape[0]
    latest = krylov_basis[-1]
    if fits_kernel(susceptibility, green_spectra):
        return fused_step(krylov_basis, susceptibility, green_spectra)
    response = convolve(latest, green_spectra)
    image = [latest[:, c] - susceptibility[None] * response[c] for c in range(3)]
    image = jnp.stack(image, axis=1)
    entry_count = 3.0 * susceptibility.size * lax.axis_size("row") * lax.axis_size("col")
    basis = krylov_basis.reshape((2 * blocks,) + image.shape[1:])
    local_coeffs = jnp.stack(
        [jnp.sum(basis * image[j][None], axis=(1, 2, 3, 4)) for j in range(2)], axis=1
    )
    coefficients = total_over_devices(local_coeffs / entry_count)
    projected = []
    for j in range(2):
        column = image[j]
        for a in range(2 * blocks):
            column = column - coefficients[a, j] * basis[a]
        projected.append(column)
    g00 = jnp.sum(projected[0] * projected[0])
    g01 = jnp.sum(projected[0] * projected[1])
    g11 = jnp.sum(projected[1] * projected[1])
    gram = total_over_devices(jnp.stack([g00, g01, g11]) / entry_count)
    lead_norm = jnp.sqrt(gram[0] + 1e-06)
    cross_term = gram[1] / lead_norm
    tail_norm = jnp.sqrt(gram[2] - cross_term * cross_term + 1e-06)
    first_column = projected[0] / lead_norm
    second_column = (projected[1] - cross_term * first_column) / tail_norm
    next_block = jnp.stack([first_column, second_column])
    block_factor = jnp.stack(
        [jnp.stack([lead_norm, cross_term]), jnp.stack([jnp.zeros_like(lead_norm), tail_norm])]
    )
    return (coefficients.reshape(blocks, 2, 2), next_block, block_factor)


def solution(mesh):
    in_specs = (
        P(None, None, None, "col", "row", None),
        P("col", "row", None),
        P(None, None, "col", "row"),
    )
    out_specs = (P(), P(None, None, "col", "row", None), P())
    return jax.shard_map(
        per_device, mesh=mesh, in_specs=in_specs, out_specs=out_specs, check_vma=False
    )
```

```python
import functools
import math

import jax
import jax.numpy as jnp
from jax import lax
from jax.experimental import pallas as pl
from jax.experimental.pallas import tpu as pltpu
from jax.sharding import PartitionSpec as P

fast = lax.Precision.HIGH
tensor_pairs = ((0, 3, 4), (3, 1, 5), (4, 5, 2))


def twiddle(count_in, count_out, period, orient, factor):
    row_index = lax.broadcasted_iota(jnp.int32, (count_in, count_out), 0)
    col_index = lax.broadcasted_iota(jnp.int32, (count_in, count_out), 1)
    phases = row_index * col_index % period
    angles = phases.astype(jnp.float32) * (2.0 * math.pi / period)
    cosine = jnp.cos(angles) * factor
    sines = jnp.sin(angles) * (orient * factor)
    return jnp.stack([jnp.stack([cosine, sines]), jnp.stack([-sines, cosine])])


def exchange_rows(blocks):
    return lax.all_to_all(blocks, "row", split_axis=0, concat_axis=0, tiled=True)


def exchange_cols(blocks):
    return lax.all_to_all(blocks, "col", split_axis=0, concat_axis=0, tiled=True)


def forward(source, table_x, table_y, table_z):
    local_z, local_y = source.shape[1:3]
    row_count, part_x = table_x.shape[-2:]
    col_count, part_y = table_y.shape[-2:]
    spectra = jnp.einsum("rzyx,rsxdl->dsyzl", source, table_x, precision=fast)
    spectra = spectra.reshape(row_count, 2, local_y, local_z * part_x)
    spectra = exchange_rows(spectra)
    spectra = spectra.transpose(1, 0, 2, 3).reshape(2, row_count * local_y, local_z, part_x)
    spectra = jnp.einsum("ryzl,rsyeq->eszql", spectra, table_y, precision=fast)
    spectra = spectra.reshape(col_count, 2, local_z, part_y * part_x)
    spectra = exchange_cols(spectra)
    spectra = spectra.transpose(1, 0, 2, 3).reshape(2, col_count * local_z, part_y * part_x)
    return jnp.einsum("rzb,rszk->skb", spectra, table_z, precision=fast)


def backward(spectra, back_x, back_y, back_z):
    row_count, part_x = back_x.shape[2:4]
    col_count, part_y, width = back_y.shape[2:]
    spectra = jnp.einsum("rkb,rskz->szb", spectra, back_z, precision=fast)
    local_z = spectra.shape[1] // col_count
    spectra = spectra.reshape(2, col_count, local_z, part_y * part_x).transpose(1, 0, 2, 3)
    spectra = exchange_cols(spectra)
    spectra = spectra.reshape(col_count, 2, local_z, part_y, part_x)
    spectra = jnp.einsum("erzql,rseqy->syzl", spectra, back_y, precision=fast)
    local_y = width // row_count
    spectra = spectra.reshape(2, row_count, local_y, local_z * part_x).transpose(1, 0, 2, 3)
    spectra = exchange_rows(spectra)
    spectra = spectra.reshape(row_count, 2, local_y, local_z, part_x)
    return jnp.einsum("dryzl,rsdlx->szyx", spectra, back_x, precision=fast)


def convolve(source, green_spectra):
    row_count = lax.axis_size("row")
    col_count = lax.axis_size("col")
    width_x = 2 * source.shape[-1]
    width_y = 2 * source.shape[-2] * row_count
    width_z = 2 * source.shape[-3] * col_count
    part_x = width_x // row_count
    part_y = width_y // col_count
    half_x, half_y, half_z = width_x // 2, width_y // 2, width_z // 2
    table_x = twiddle(half_x, width_x, width_x, -1.0, 1.0).reshape(2, 2, half_x, row_count, part_x)
    table_y = twiddle(half_y, width_y, width_y, -1.0, 1.0).reshape(2, 2, half_y, col_count, part_y)
    table_z = twiddle(half_z, width_z, width_z, -1.0, 1.0)
    spectra = [forward(source[:, c], table_x, table_y, table_z) for c in range(3)]
    coupling = green_spectra.astype(jnp.float32).reshape(6, width_z, part_y * part_x)
    back_z = twiddle(width_z, half_z, width_z, 1.0, 1.0)
    back_y = twiddle(width_y, half_y, width_y, 1.0, 1.0).reshape(2, 2, col_count, part_y, half_y)
    scaling = 1.0 / (width_x * width_y * width_z)
    back_x = twiddle(width_x, half_x, width_x, 1.0, scaling).reshape(2, 2, row_count, part_x, half_x)
    result = []
    for member in range(3):
        chosen = tensor_pairs[member]
        total = coupling[chosen[0]] * spectra[0]
        total = total + coupling[chosen[1]] * spectra[1]
        total = total + coupling[chosen[2]] * spectra[2]
        result.append(backward(total, back_x, back_y, back_z))
    return result


LANES = 128
SLABS = 4
AHEAD = 2
LAG = 2
MESH = pl.DeviceIdType.MESH


def cosine_of(phase, period):
    quarter = period // 4
    turn = (phase + quarter // 2) // quarter
    angle = (phase - turn * quarter).astype(jnp.float32) * (2.0 * math.pi / period)
    square = angle * angle
    even = 1.0 / 24 - square * (1.0 / 720 - square * (1.0 / 40320))
    even = 1.0 - square * (0.5 - square * even)
    odd = 1.0 / 120 - square * (1.0 / 5040 - square * (1.0 / 362880))
    odd = angle * (1.0 - square * (1.0 / 6 - square * odd))
    value = jnp.where(turn % 2 == 0, even, odd)
    return jnp.where((turn + 1) % 4 < 2, value, -value)


def halves(value):
    high = value.astype(jnp.bfloat16)
    return high, (value - high.astype(jnp.float32)).astype(jnp.bfloat16)


def iota(shape, axis):
    return lax.broadcasted_iota(jnp.int32, shape, axis)


def swap_lanes(first, second):
    last = first.ndim - 1
    lane = lax.broadcasted_iota(jnp.int32, first.shape, last)
    keep = lane % 64 < 32
    return (
        jnp.where(keep, first, pltpu.roll(second, 32, last)),
        jnp.where(keep, pltpu.roll(first, 96, last), second),
    )


def stacked_operand(column):
    sign = jnp.where(iota(column.shape, 1) < 64, 1.0, -1.0)
    high, low = halves(jnp.concatenate([column, pltpu.roll(column, 64, 1) * sign], axis=0))
    return jnp.concatenate([high, low, high], axis=0)


def left_product(table, columns):
    operand = jnp.concatenate([stacked_operand(column) for column in columns], axis=1)
    return jnp.dot(table, operand, preferred_element_type=jnp.float32)


def right_product(rows, table_high, table_low, flip):
    dims = (((1,), (1,) if flip else (0,)), ((), ()))
    high, low = halves(rows)
    both = jnp.concatenate([high, low], axis=0)
    main = lax.dot_general(both, table_high, dims, preferred_element_type=jnp.float32)
    rest = lax.dot_general(high, table_low, dims, preferred_element_type=jnp.float32)
    count = rows.shape[0]
    return main[:count] + (main[count:] + rest)


def field_kernel(
    row_count,
    col_count,
    krylov,
    chi,
    green,
    projected,
    coefficients,
    factor,
    grid_a,
    grid_b,
    grid_c,
    grid_d,
    line_table,
    ahead_table,
    back_table,
    basis,
    chi_all,
    image,
    green_slot,
    weights,
    mixed,
    sums,
    gather_one,
    gather_two,
    f1s, f1r, f1l, f2s, f2r, f2l, b1s, b1r, b1l, b2s, b2r, b2l,
    green_sem,
    basis_sem,
    source_sem,
    chi_sem,
    out_sem,
    gather_send,
    gather_recv,
    row_credit,
    col_credit,
):
    blocks = krylov.shape[0]
    local_z, local_y, half_x = chi.shape
    pairs_y = grid_c.shape[4]
    full_z = green.shape[3]
    half_y = local_y * row_count
    part_x = green.shape[2]
    world = row_count * col_count
    depth = local_z // SLABS
    pair_depth = depth // 2
    chunks = 3 * SLABS
    units = pairs_y // 2
    me_row = lax.axis_index("row")
    me_col = lax.axis_index("col")

    def where_of(k):
        return k // SLABS, k % SLABS

    barrier = pltpu.get_barrier_semaphore()
    me = me_row * col_count + me_col

    def others(body):
        for i in range(row_count):
            for j in range(col_count):
                if i or j:
                    peer_row = lax.rem(me_row + i, row_count)
                    peer_col = lax.rem(me_col + j, col_count)
                    body({"row": peer_row, "col": peer_col})

    others(lambda peer: pl.semaphore_signal(barrier, 1, device_id=peer, device_id_type=MESH))

    source = basis.at[blocks - 1]

    def source_copy(c):
        return pltpu.make_async_copy(krylov.at[blocks - 1, :, c], source.at[:, c], source_sem.at[c])

    older = pltpu.make_async_copy(
        krylov.at[pl.ds(0, blocks - 1)], basis.at[pl.ds(0, blocks - 1)], basis_sem
    )
    chi_copy = pltpu.make_async_copy(chi, chi_all, chi_sem)

    def out_copy(c):
        return pltpu.make_async_copy(image.at[:, c], projected.at[:, c], out_sem.at[c])

    def green_copies(i):
        slot = i % 2
        h = i // units
        pair = i % units * 2
        return [
            pltpu.make_async_copy(
                green.at[:, pl.ds(half * pairs_y + pair, 2), pl.ds(h * 32, 32)],
                green_slot.at[slot, half],
                green_sem.at[slot, half],
            )
            for half in range(2)
        ]

    def build_line_table(h):
        rows = 64
        def step(t, carry):
            shape = (rows, row_count * part_x)
            row = iota(shape, 0) + t * rows
            col = iota(shape, 1)
            point = row % half_x
            freq = col // LANES * (2 * part_x) + col // 32 % 2 * part_x + h * 32 + col % 32
            turn = col // 64 % 2 - row // half_x
            phase = (point * freq + (turn + 4) * (half_x // 2)) % (2 * half_x)
            high, low = halves(cosine_of(phase, 2 * half_x))
            line_table[h, 0, pl.ds(t * rows, rows)] = high
            line_table[h, 1, pl.ds(t * rows, rows)] = low
            return carry

        lax.fori_loop(0, 2 * half_x // rows, step, 0)

    def build_left_tables():
        rows = 64

        def step(t, carry):
            shape = (rows, 2 * half_y)
            freq = iota(shape, 0) + t * rows
            col = iota(shape, 1)
            phase = freq * (col % half_y) + (4 - col // half_y) * (half_y // 2)
            high, low = halves(cosine_of(phase % (2 * half_y), 2 * half_y))
            ahead_table[pl.ds(t * rows, rows)] = jnp.concatenate([high, high, low], axis=1)
            return carry

        lax.fori_loop(0, 2 * half_y // rows, step, 0)

        def back_step(t, carry):
            shape = (rows, 4 * half_y)
            point = iota(shape, 0) + t * rows
            col = iota(shape, 1)
            phase = point * (col % (2 * half_y)) + col // (2 * half_y) * (half_y // 2)
            high, low = halves(cosine_of(phase % (2 * half_y), 2 * half_y))
            back_table[pl.ds(t * rows, rows)] = jnp.concatenate([high, high, low], axis=1)
            return carry

        lax.fori_loop(0, half_y // rows, back_step, 0)

    def send(axis, count, me, src, dst, send_sem, recv_sem, local_sem):
        for step in range(1, count):
            peer = lax.rem(me + step, count)
            pltpu.make_async_remote_copy(
                src_ref=src(peer),
                dst_ref=dst(me),
                send_sem=send_sem,
                recv_sem=recv_sem,
                device_id={axis: peer},
                device_id_type=MESH,
            ).start()
        pltpu.make_async_copy(src(me), dst(me), local_sem).start()

    def row_part(grid, h, k):
        c, q = where_of(k)
        return lambda p: grid.at[h, p, c, pl.ds(q * pair_depth, pair_depth)]

    def col_part(grid, h, k):
        c, q = where_of(k)
        return lambda j: grid.at[h, j, c, pl.ds(q * depth, depth)]

    def many(grid, h, k, count, size):
        c, q = where_of(k)
        return grid.at[h, pl.ds(0, count - 1), c, pl.ds(q * size, size)]

    def wait_bytes(ref, sem):
        pltpu.make_async_copy(ref, ref, sem).wait()

    def wait_row(grid, h, k, recv, local):
        n = h * chunks + k
        wait_bytes(many(grid, h, k, row_count, pair_depth), recv.at[n])
        wait_bytes(row_part(grid, h, k)(me_row), local.at[n])

    def wait_col(grid, h, k, recv, local):
        n = h * chunks + k
        wait_bytes(many(grid, h, k, col_count, depth), recv.at[n])
        wait_bytes(col_part(grid, h, k)(me_col), local.at[n])

    def send_row(src, dst, h, k, sems):
        n = h * chunks + k
        send("row", row_count, me_row, row_part(src, h, k), row_part(dst, h, k),
             sems[0].at[n], sems[1].at[n], sems[2].at[n])

    def send_col(src, dst, h, k, sems):
        n = h * chunks + k
        send("col", col_count, me_col, col_part(src, h, k), col_part(dst, h, k),
             sems[0].at[n], sems[1].at[n], sems[2].at[n])

    def ahead_lines(h, k):
        c, q = where_of(k)
        rows = []
        for zb in range(2):
            members = [
                jnp.concatenate(
                    [source[r, c, q * depth + 2 * z + zb] for z in range(pair_depth)], axis=0
                )
                for r in range(2)
            ]
            rows.append(jnp.concatenate(members, axis=1))
        result = right_product(
            jnp.concatenate(rows, axis=0), line_table[h, 0], line_table[h, 1], False
        )
        count = pair_depth * local_y
        for pp in range(row_count // 2):
            part = result[:, pp * LANES : (pp + 1) * LANES]
            first, second = swap_lanes(part[:count], part[count:])
            for b, value in ((0, first), (1, second)):
                grid_a[h, 2 * pp + b, c, pl.ds(q * pair_depth, pair_depth)] = value.reshape(
                    pair_depth, local_y, LANES
                )
        send_row(grid_a, grid_b, h, k, (f1s, f1r, f1l))

    def ahead_columns(h, k):
        c, q = where_of(k)
        wait_row(grid_b, h, k, f1r, f1l)

        def step(t, carry):
            z0 = q * pair_depth + 2 * t
            columns = [
                grid_b[h, :, c, z0 + i].reshape(row_count * local_y, LANES) for i in range(2)
            ]
            result = left_product(ahead_table[...], columns)
            for i in range(2):
                part = result[:, i * LANES : (i + 1) * LANES]
                part = part.reshape(col_count, 2, pairs_y, LANES)
                first, second = swap_lanes(part[:, 0], part[:, 1])
                grid_c[h, :, c, 2 * (z0 + i)] = first
                grid_c[h, :, c, 2 * (z0 + i) + 1] = second
            return carry

        lax.fori_loop(0, pair_depth // 2, step, 0)
        send_col(grid_c, grid_d, h, k, (f2s, f2r, f2l))

    def mix(h, unit):
        step = h * units + unit
        slot = step % 2
        ky = unit * 2
        flat = [
            [grid_d.at[h, j, c].reshape(local_z * pairs_y, LANES) for c in range(3)]
            for j in range(col_count)
        ]
        for c in range(3):
            columns = []
            for i in range(2):
                pieces = [
                    flat[j][c][pl.ds(ky + i, local_z, stride=pairs_y), :] for j in range(col_count)
                ]
                columns.append(jnp.concatenate(pieces, axis=0))
            mixed[c] = left_product(ahead_table[...], columns)
        for copy in green_copies(step):
            copy.wait()
        for entry in range(6):
            for i in range(2):
                first = green_slot[slot, 0, entry, i]
                second = green_slot[slot, 1, entry, i]
                block = jnp.concatenate([first, second, first, second], axis=0)
                weights[entry, :, i * LANES : (i + 1) * LANES] = block.T.astype(jnp.float32)

        @pl.when(step + 2 < 2 * units)
        def _():
            for copy in green_copies(step + 2):
                copy.start()

        for c in range(3):
            columns = []
            for i in range(2):
                part = slice(i * LANES, (i + 1) * LANES)
                total = None
                for other in range(3):
                    term = weights[tensor_pairs[c][other], :, part] * mixed[other, :, part]
                    total = term if total is None else total + term
                columns.append(total)
            result = left_product(back_table[...], columns)
            for i in range(2):
                for j in range(col_count):
                    flat[j][c][pl.ds(ky + i, local_z, stride=pairs_y), :] = result[
                        j * local_z : (j + 1) * local_z, i * LANES : (i + 1) * LANES
                    ]

    def mix_some(h, turn, turns):
        def step(unit, carry):
            mix(h, unit)
            return carry

        low = jnp.clip(turn, 0, turns) * units // turns
        lax.fori_loop(low, jnp.clip(turn + 1, 0, turns) * units // turns, step, 0)

    def back_columns(h, k):
        c, q = where_of(k)

        def step(t, carry):
            z0 = q * pair_depth + 2 * t
            columns = []
            for i in range(2):
                first, second = swap_lanes(
                    grid_c[h, :, c, 2 * (z0 + i)], grid_c[h, :, c, 2 * (z0 + i) + 1]
                )
                pieces = []
                for j in range(col_count):
                    pieces += [first[j], second[j]]
                columns.append(jnp.concatenate(pieces, axis=0))
            result = left_product(back_table[...], columns)
            for i in range(2):
                part = result[:, i * LANES : (i + 1) * LANES]
                grid_b[h, :, c, z0 + i] = part.reshape(row_count, local_y, LANES)
            return carry

        lax.fori_loop(0, pair_depth // 2, step, 0)
        send_row(grid_b, grid_a, h, k, (b2s, b2r, b2l))

    scaling = 1.0 / (4.0 * half_x * half_y * full_z)

    def back_lines(k):
        c, q = where_of(k)
        for h in range(2):
            wait_row(grid_a, h, k, b2r, b2l)
        count = pair_depth * local_y
        result = None
        for h in range(2):
            low, high = [], []
            for pp in range(row_count // 2):
                values = [
                    grid_a[h, 2 * pp + b, c, pl.ds(q * pair_depth, pair_depth)].reshape(count, LANES)
                    for b in range(2)
                ]
                first, second = swap_lanes(*values)
                low.append(first)
                high.append(second)
            rows = jnp.concatenate(
                [jnp.concatenate(low, axis=1), jnp.concatenate(high, axis=1)], axis=0
            )
            term = right_product(rows, line_table[h, 0], line_table[h, 1], True)
            result = term if result is None else result + term
        partial = [None] * (4 * blocks)
        for zb in range(2):
            for pair in range(pair_depth):
                z = q * depth + 2 * pair + zb
                start = zb * count + pair * local_y
                weight = chi_all[z] * scaling
                columns = []
                for r in range(2):
                    value = (
                        source[r, c, z]
                        - weight * result[start : start + local_y, r * half_x : (r + 1) * half_x]
                    )
                    image[r, c, z] = value
                    columns.append(value)
                for a in range(2 * blocks):
                    member = basis[a // 2, a % 2, c, z]
                    for r in range(2):
                        term = fold(member * columns[r])
                        old = partial[2 * a + r]
                        partial[2 * a + r] = term if old is None else old + term
        for i in range(4 * blocks):
            sums[i] = sums[i] + partial[i]

    def exchange(gather, n):
        def start(peer):
            pltpu.make_async_remote_copy(
                src_ref=gather.at[me],
                dst_ref=gather.at[me],
                send_sem=gather_send.at[n],
                recv_sem=gather_recv.at[n],
                device_id=peer,
                device_id_type=MESH,
            ).start()

        others(start)
        rest = gather.at[pl.ds(0, world - 1)]
        wait_bytes(rest, gather_recv.at[n])
        wait_bytes(rest, gather_send.at[n])
        total = gather[0]
        for i in range(1, world):
            total = total + gather[i]
        return jnp.sum(total, axis=1, keepdims=True) * (1.0 / (3.0 * chi_all.size * world))

    def orthonormalize():
        gather_one[me] = jnp.sum(sums[...], axis=1)
        products = exchange(gather_one, 0)
        coefficients[...] = jnp.broadcast_to(products, coefficients.shape)
        zero = jnp.zeros((8, LANES), jnp.float32)

        def project(z, totals):
            totals = list(totals)
            for c in range(3):
                columns = [image[r, c, z] for r in range(2)]
                for a in range(2 * blocks):
                    member = basis[a // 2, a % 2, c, z]
                    for r in range(2):
                        i = 2 * a + r
                        columns[r] = columns[r] - products[i : i + 1] * member
                for r in range(2):
                    image[r, c, z] = columns[r]
                for n, (i, j) in enumerate(((0, 0), (0, 1), (1, 1))):
                    totals[n] = totals[n] + fold(columns[i] * columns[j])
            return tuple(totals)

        totals = lax.fori_loop(0, local_z, project, (zero, zero, zero))
        for c in range(3):
            out_copy(c).start()
        rows = [jnp.sum(total, axis=0, keepdims=True) for total in totals]
        gather_two[me] = jnp.concatenate(rows + [zero[:5]], axis=0)
        gram = exchange(gather_two, 1)
        lead = jnp.sqrt(gram[0:1] + 1e-06)
        cross = gram[1:2] / lead
        tail = jnp.sqrt(gram[2:3] - cross * cross + 1e-06)
        values = jnp.concatenate([lead, cross, zero[:1, :1], tail, zero[:4, :1]], axis=0)
        factor[...] = jnp.broadcast_to(values, factor.shape)
        for c in range(3):
            out_copy(c).wait()

    def fold(value):
        total = None
        for i in range(local_y // 8):
            for j in range(half_x // LANES):
                piece = value[i * 8 : (i + 1) * 8, j * LANES : (j + 1) * LANES]
                total = piece if total is None else total + piece
        return total

    def loop(body):
        def step(k, carry):
            body(k)
            return carry

        lax.fori_loop(0, chunks, step, 0)

    for c in range(3):
        source_copy(c).start()
    for i in range(2):
        for copy in green_copies(i):
            copy.start()
    chi_copy.start()
    older.start()
    build_line_table(0)
    sums[...] = jnp.zeros(sums.shape, jnp.float32)
    for c in range(3):
        source_copy(c).wait()
    pl.semaphore_wait(barrier, world - 1)
    def ahead_send(n):
        ahead_lines(n // chunks, n % chunks)

    def back_send(n):
        send_col(grid_d, grid_c, n // chunks, n % chunks, (b1s, b1r, b1l))

    for n in range(AHEAD):
        ahead_send(jnp.int32(n))
    build_left_tables()
    build_line_table(1)

    def free_rows(k):
        for h in range(2):
            wait_bytes(many(grid_a, h, k, row_count, pair_depth), f1s.at[h * chunks + k])

    def free_cols(h):
        loop(lambda k: wait_bytes(many(grid_c, h, k, col_count, depth), f2s.at[h * chunks + k]))
        for step in range(1, col_count):
            peer = lax.rem(me_col + step, col_count)
            pl.semaphore_signal(
                col_credit.at[h], 1, device_id={"col": peer}, device_id_type=MESH
            )

    def first_half(n, carry):
        ahead_columns(n // chunks, n % chunks)

        @pl.when(n + AHEAD < 2 * chunks)
        def _():
            ahead_send(n + AHEAD)

        @pl.when(n == chunks)
        def _():
            loop(lambda k: wait_col(grid_d, 0, k, f2r, f2l))

        mix_some(0, n - chunks, chunks - 1)
        return carry

    lax.fori_loop(0, 2 * chunks, first_half, 0)
    free_cols(0)
    pl.semaphore_wait(col_credit.at[0], col_count - 1)
    for n in range(AHEAD):
        back_send(jnp.int32(n))
    loop(free_rows)
    for step in range(1, row_count):
        peer = lax.rem(me_row + step, row_count)
        pl.semaphore_signal(row_credit, 1, device_id={"row": peer}, device_id_type=MESH)
    loop(lambda k: wait_col(grid_d, 1, k, f2r, f2l))
    free_cols(1)
    chi_copy.wait()
    older.wait()
    pl.semaphore_wait(row_credit, row_count - 1)
    pl.semaphore_wait(col_credit.at[1], col_count - 1)

    def second_half(n, carry):
        h, k = n // chunks, n % chunks
        wait_col(grid_c, h, k, b1r, b1l)

        @pl.when(n + AHEAD < 2 * chunks)
        def _():
            back_send(n + AHEAD)

        back_columns(h, k)
        mix_some(1, n, chunks - AHEAD)

        @pl.when(n >= chunks + LAG)
        def _():
            back_lines(n - chunks - LAG)

        return carry

    lax.fori_loop(0, 2 * chunks, second_half, 0)
    for k in range(chunks - LAG, chunks):
        back_lines(jnp.int32(k))
    orthonormalize()

    def finish(k):
        for h in range(2):
            n = h * chunks + k
            wait_bytes(many(grid_d, h, k, col_count, depth), b1s.at[n])
            wait_bytes(many(grid_b, h, k, row_count, pair_depth), b2s.at[n])

    loop(finish)


def fits_kernel(susceptibility, green_spectra):
    local_z, local_y, half_x = susceptibility.shape
    full_z, part_y, part_x = green_spectra.shape[1:]
    return (
        part_x == LANES // 2
        and part_y % 16 == 0
        and full_z % LANES == 0
        and full_z == 2 * local_y * lax.axis_size("row")
        and local_y % 8 == 0
        and local_z % (4 * SLABS) == 0
        and half_x % LANES == 0
        and lax.axis_size("row") % 2 == 0
    )


def fused_step(krylov_basis, susceptibility, green_spectra):
    row_count = lax.axis_size("row")
    col_count = lax.axis_size("col")
    world = row_count * col_count
    blocks = krylov_basis.shape[0]
    local_z, local_y, half_x = susceptibility.shape
    full_z, part_y, part_x = green_spectra.shape[1:]
    half_y = local_y * row_count
    pairs_y = part_y // 2
    row_grid = pltpu.VMEM((2, row_count, 3, local_z // 2, local_y, LANES), jnp.float32)
    col_grid = pltpu.VMEM((2, col_count, 3, local_z, pairs_y, LANES), jnp.float32)
    dma = pltpu.SemaphoreType.DMA
    whole = pl.BlockSpec(memory_space=pltpu.VMEM)
    outside = pl.BlockSpec(memory_space=pl.ANY)
    field = (2, 3, local_z, local_y, half_x)
    projected, coefficients, factor = pl.pallas_call(
        functools.partial(field_kernel, row_count, col_count),
        out_shape=(
            jax.ShapeDtypeStruct(field, jnp.float32),
            jax.ShapeDtypeStruct((4 * blocks, LANES), jnp.float32),
            jax.ShapeDtypeStruct((8, LANES), jnp.float32),
        ),
        in_specs=[outside] * 3,
        out_specs=(outside, whole, whole),
        scratch_shapes=[
            row_grid,
            row_grid,
            col_grid,
            col_grid,
            pltpu.VMEM((2, 2, 2 * half_x, row_count * part_x), jnp.bfloat16),
            pltpu.VMEM((2 * half_y, 6 * half_y), jnp.bfloat16),
            pltpu.VMEM((half_y, 12 * half_y), jnp.bfloat16),
            pltpu.VMEM((blocks,) + field, jnp.float32),
            pltpu.VMEM((local_z, local_y, half_x), jnp.float32),
            pltpu.VMEM(field, jnp.float32),
            pltpu.VMEM((2, 2, 6, 2, 32, full_z), jnp.bfloat16),
            pltpu.VMEM((6, full_z, 2 * LANES), jnp.float32),
            pltpu.VMEM((3, full_z, 2 * LANES), jnp.float32),
            pltpu.VMEM((4 * blocks, 8, LANES), jnp.float32),
            pltpu.VMEM((world, 4 * blocks, LANES), jnp.float32),
            pltpu.VMEM((world, 8, LANES), jnp.float32),
        ]
        + [dma((2 * 3 * SLABS,))] * 12
        + [
            dma((2, 2)),
            dma,
            dma((3,)),
            dma,
            dma((3,)),
            dma((2,)),
            dma((2,)),
            pltpu.SemaphoreType.REGULAR,
            pltpu.SemaphoreType.REGULAR((2,)),
        ],
        compiler_params=pltpu.CompilerParams(
            collective_id=0, has_side_effects=True, vmem_limit_bytes=67043328
        ),
        name="fused_step",
    )(krylov_basis, susceptibility, green_spectra.transpose(0, 2, 3, 1))
    projections = coefficients[:, 0].reshape(blocks, 2, 2)
    block_factor = factor[:4, 0].reshape(2, 2)
    first = projected[0] * (1.0 / factor[0, 0])
    second = (projected[1] - factor[1, 0] * first) * (1.0 / factor[3, 0])
    return projections, jnp.stack([first, second]), block_factor


def total_over_devices(partial):
    return jnp.sum(lax.all_gather(partial, ("row", "col")), axis=0)


def per_device(krylov_basis, susceptibility, green_spectra):
    blocks = krylov_basis.shape[0]
    latest = krylov_basis[-1]
    if fits_kernel(susceptibility, green_spectra):
        return fused_step(krylov_basis, susceptibility, green_spectra)
    response = convolve(latest, green_spectra)
    image = [latest[:, c] - susceptibility[None] * response[c] for c in range(3)]
    image = jnp.stack(image, axis=1)
    entry_count = 3.0 * susceptibility.size * lax.axis_size("row") * lax.axis_size("col")
    basis = krylov_basis.reshape((2 * blocks,) + image.shape[1:])
    local_coeffs = jnp.stack(
        [jnp.sum(basis * image[j][None], axis=(1, 2, 3, 4)) for j in range(2)], axis=1
    )
    coefficients = total_over_devices(local_coeffs / entry_count)
    projected = []
    for j in range(2):
        column = image[j]
        for a in range(2 * blocks):
            column = column - coefficients[a, j] * basis[a]
        projected.append(column)
    g00 = jnp.sum(projected[0] * projected[0])
    g01 = jnp.sum(projected[0] * projected[1])
    g11 = jnp.sum(projected[1] * projected[1])
    gram = total_over_devices(jnp.stack([g00, g01, g11]) / entry_count)
    lead_norm = jnp.sqrt(gram[0] + 1e-06)
    cross_term = gram[1] / lead_norm
    tail_norm = jnp.sqrt(gram[2] - cross_term * cross_term + 1e-06)
    first_column = projected[0] / lead_norm
    second_column = (projected[1] - cross_term * first_column) / tail_norm
    next_block = jnp.stack([first_column, second_column])
    block_factor = jnp.stack(
        [jnp.stack([lead_norm, cross_term]), jnp.stack([jnp.zeros_like(lead_norm), tail_norm])]
    )
    return (coefficients.reshape(blocks, 2, 2), next_block, block_factor)


def solution(mesh):
    in_specs = (
        P(None, None, None, "col", "row", None),
        P("col", "row", None),
        P(None, None, "col", "row"),
    )
    out_specs = (P(), P(None, None, "col", "row", None), P())
    return jax.shard_map(
        per_device, mesh=mesh, in_specs=in_specs, out_specs=out_specs, check_vma=False
    )
```

```python
import functools
import math

import jax
import jax.numpy as jnp
from jax import lax
from jax.experimental import pallas as pl
from jax.experimental.pallas import tpu as pltpu
from jax.sharding import PartitionSpec as P

fast = lax.Precision.HIGH
tensor_pairs = ((0, 3, 4), (3, 1, 5), (4, 5, 2))


def twiddle(count_in, count_out, period, orient, factor):
    row_index = lax.broadcasted_iota(jnp.int32, (count_in, count_out), 0)
    col_index = lax.broadcasted_iota(jnp.int32, (count_in, count_out), 1)
    phases = row_index * col_index % period
    angles = phases.astype(jnp.float32) * (2.0 * math.pi / period)
    cosine = jnp.cos(angles) * factor
    sines = jnp.sin(angles) * (orient * factor)
    return jnp.stack([jnp.stack([cosine, sines]), jnp.stack([-sines, cosine])])


def exchange_rows(blocks):
    return lax.all_to_all(blocks, "row", split_axis=0, concat_axis=0, tiled=True)


def exchange_cols(blocks):
    return lax.all_to_all(blocks, "col", split_axis=0, concat_axis=0, tiled=True)


def forward(source, table_x, table_y, table_z):
    local_z, local_y = source.shape[1:3]
    row_count, part_x = table_x.shape[-2:]
    col_count, part_y = table_y.shape[-2:]
    spectra = jnp.einsum("rzyx,rsxdl->dsyzl", source, table_x, precision=fast)
    spectra = spectra.reshape(row_count, 2, local_y, local_z * part_x)
    spectra = exchange_rows(spectra)
    spectra = spectra.transpose(1, 0, 2, 3).reshape(2, row_count * local_y, local_z, part_x)
    spectra = jnp.einsum("ryzl,rsyeq->eszql", spectra, table_y, precision=fast)
    spectra = spectra.reshape(col_count, 2, local_z, part_y * part_x)
    spectra = exchange_cols(spectra)
    spectra = spectra.transpose(1, 0, 2, 3).reshape(2, col_count * local_z, part_y * part_x)
    return jnp.einsum("rzb,rszk->skb", spectra, table_z, precision=fast)


def backward(spectra, back_x, back_y, back_z):
    row_count, part_x = back_x.shape[2:4]
    col_count, part_y, width = back_y.shape[2:]
    spectra = jnp.einsum("rkb,rskz->szb", spectra, back_z, precision=fast)
    local_z = spectra.shape[1] // col_count
    spectra = spectra.reshape(2, col_count, local_z, part_y * part_x).transpose(1, 0, 2, 3)
    spectra = exchange_cols(spectra)
    spectra = spectra.reshape(col_count, 2, local_z, part_y, part_x)
    spectra = jnp.einsum("erzql,rseqy->syzl", spectra, back_y, precision=fast)
    local_y = width // row_count
    spectra = spectra.reshape(2, row_count, local_y, local_z * part_x).transpose(1, 0, 2, 3)
    spectra = exchange_rows(spectra)
    spectra = spectra.reshape(row_count, 2, local_y, local_z, part_x)
    return jnp.einsum("dryzl,rsdlx->szyx", spectra, back_x, precision=fast)


def convolve(source, green_spectra):
    row_count = lax.axis_size("row")
    col_count = lax.axis_size("col")
    width_x = 2 * source.shape[-1]
    width_y = 2 * source.shape[-2] * row_count
    width_z = 2 * source.shape[-3] * col_count
    part_x = width_x // row_count
    part_y = width_y // col_count
    half_x, half_y, half_z = width_x // 2, width_y // 2, width_z // 2
    table_x = twiddle(half_x, width_x, width_x, -1.0, 1.0).reshape(2, 2, half_x, row_count, part_x)
    table_y = twiddle(half_y, width_y, width_y, -1.0, 1.0).reshape(2, 2, half_y, col_count, part_y)
    table_z = twiddle(half_z, width_z, width_z, -1.0, 1.0)
    spectra = [forward(source[:, c], table_x, table_y, table_z) for c in range(3)]
    coupling = green_spectra.astype(jnp.float32).reshape(6, width_z, part_y * part_x)
    back_z = twiddle(width_z, half_z, width_z, 1.0, 1.0)
    back_y = twiddle(width_y, half_y, width_y, 1.0, 1.0).reshape(2, 2, col_count, part_y, half_y)
    scaling = 1.0 / (width_x * width_y * width_z)
    back_x = twiddle(width_x, half_x, width_x, 1.0, scaling).reshape(2, 2, row_count, part_x, half_x)
    result = []
    for member in range(3):
        chosen = tensor_pairs[member]
        total = coupling[chosen[0]] * spectra[0]
        total = total + coupling[chosen[1]] * spectra[1]
        total = total + coupling[chosen[2]] * spectra[2]
        result.append(backward(total, back_x, back_y, back_z))
    return result


LANES = 128
SLABS = 8
AHEAD = 3
LAG = 3
MESH = pl.DeviceIdType.MESH


def cosine_of(phase, period):
    quarter = period // 4
    turn = (phase + quarter // 2) // quarter
    angle = (phase - turn * quarter).astype(jnp.float32) * (2.0 * math.pi / period)
    square = angle * angle
    even = 1.0 / 24 - square * (1.0 / 720 - square * (1.0 / 40320))
    even = 1.0 - square * (0.5 - square * even)
    odd = 1.0 / 120 - square * (1.0 / 5040 - square * (1.0 / 362880))
    odd = angle * (1.0 - square * (1.0 / 6 - square * odd))
    value = jnp.where(turn % 2 == 0, even, odd)
    return jnp.where((turn + 1) % 4 < 2, value, -value)


def halves(value):
    high = value.astype(jnp.bfloat16)
    return high, (value - high.astype(jnp.float32)).astype(jnp.bfloat16)


def iota(shape, axis):
    return lax.broadcasted_iota(jnp.int32, shape, axis)


def swap_lanes(first, second):
    last = first.ndim - 1
    lane = lax.broadcasted_iota(jnp.int32, first.shape, last)
    keep = lane % 64 < 32
    return (
        jnp.where(keep, first, pltpu.roll(second, 32, last)),
        jnp.where(keep, pltpu.roll(first, 96, last), second),
    )


def stacked_operand(column):
    sign = jnp.where(iota(column.shape, 1) < 64, 1.0, -1.0)
    high, low = halves(jnp.concatenate([column, pltpu.roll(column, 64, 1) * sign], axis=0))
    return jnp.concatenate([high, low, high], axis=0)


def left_product(table, columns):
    operand = jnp.concatenate([stacked_operand(column) for column in columns], axis=1)
    return jnp.dot(table, operand, preferred_element_type=jnp.float32)


def right_product(rows, table_high, table_low, flip):
    dims = (((1,), (1,) if flip else (0,)), ((), ()))
    high, low = halves(rows)
    both = jnp.concatenate([high, low], axis=0)
    main = lax.dot_general(both, table_high, dims, preferred_element_type=jnp.float32)
    rest = lax.dot_general(high, table_low, dims, preferred_element_type=jnp.float32)
    count = rows.shape[0]
    return main[:count] + (main[count:] + rest)


def field_kernel(
    row_count,
    col_count,
    krylov,
    chi,
    green,
    projected,
    coefficients,
    factor,
    grid_a,
    grid_b,
    grid_c,
    grid_d,
    line_table,
    ahead_table,
    back_table,
    basis,
    chi_all,
    image,
    green_slot,
    weights,
    mixed,
    sums,
    gather_one,
    gather_two,
    f1s, f1r, f1l, f2s, f2r, f2l, b1s, b1r, b1l, b2s, b2r, b2l,
    green_sem,
    basis_sem,
    source_sem,
    chi_sem,
    out_sem,
    gather_send,
    gather_recv,
    row_credit,
    col_credit,
):
    blocks = krylov.shape[0]
    local_z, local_y, half_x = chi.shape
    pairs_y = grid_c.shape[4]
    full_z = green.shape[3]
    half_y = local_y * row_count
    part_x = green.shape[2]
    world = row_count * col_count
    depth = local_z // SLABS
    pair_depth = depth // 2
    chunks = 3 * SLABS
    units = pairs_y // 2
    me_row = lax.axis_index("row")
    me_col = lax.axis_index("col")

    def where_of(k):
        return k // SLABS, k % SLABS

    barrier = pltpu.get_barrier_semaphore()
    me = me_row * col_count + me_col

    def others(body):
        for i in range(row_count):
            for j in range(col_count):
                if i or j:
                    peer_row = lax.rem(me_row + i, row_count)
                    peer_col = lax.rem(me_col + j, col_count)
                    body({"row": peer_row, "col": peer_col})

    others(lambda peer: pl.semaphore_signal(barrier, 1, device_id=peer, device_id_type=MESH))

    source = basis.at[blocks - 1]

    def source_copy(c):
        return pltpu.make_async_copy(krylov.at[blocks - 1, :, c], source.at[:, c], source_sem.at[c])

    older = pltpu.make_async_copy(
        krylov.at[pl.ds(0, blocks - 1)], basis.at[pl.ds(0, blocks - 1)], basis_sem
    )
    chi_copy = pltpu.make_async_copy(chi, chi_all, chi_sem)

    def out_copy(c):
        return pltpu.make_async_copy(image.at[:, c], projected.at[:, c], out_sem.at[c])

    def green_copies(i):
        slot = i % 2
        h = i // units
        pair = i % units * 2
        return [
            pltpu.make_async_copy(
                green.at[:, pl.ds(half * pairs_y + pair, 2), pl.ds(h * 32, 32)],
                green_slot.at[slot, half],
                green_sem.at[slot, half],
            )
            for half in range(2)
        ]

    def build_line_table(h):
        rows = 64
        def step(t, carry):
            shape = (rows, row_count * part_x)
            row = iota(shape, 0) + t * rows
            col = iota(shape, 1)
            point = row % half_x
            freq = col // LANES * (2 * part_x) + col // 32 % 2 * part_x + h * 32 + col % 32
            turn = col // 64 % 2 - row // half_x
            phase = (point * freq + (turn + 4) * (half_x // 2)) % (2 * half_x)
            high, low = halves(cosine_of(phase, 2 * half_x))
            line_table[h, 0, pl.ds(t * rows, rows)] = high
            line_table[h, 1, pl.ds(t * rows, rows)] = low
            return carry

        lax.fori_loop(0, 2 * half_x // rows, step, 0)

    def build_left_tables():
        rows = 64

        def step(t, carry):
            shape = (rows, 2 * half_y)
            freq = iota(shape, 0) + t * rows
            col = iota(shape, 1)
            phase = freq * (col % half_y) + (4 - col // half_y) * (half_y // 2)
            high, low = halves(cosine_of(phase % (2 * half_y), 2 * half_y))
            ahead_table[pl.ds(t * rows, rows)] = jnp.concatenate([high, high, low], axis=1)
            return carry

        lax.fori_loop(0, 2 * half_y // rows, step, 0)

        def back_step(t, carry):
            shape = (rows, 4 * half_y)
            point = iota(shape, 0) + t * rows
            col = iota(shape, 1)
            phase = point * (col % (2 * half_y)) + col // (2 * half_y) * (half_y // 2)
            high, low = halves(cosine_of(phase % (2 * half_y), 2 * half_y))
            back_table[pl.ds(t * rows, rows)] = jnp.concatenate([high, high, low], axis=1)
            return carry

        lax.fori_loop(0, half_y // rows, back_step, 0)

    def send(axis, count, me, src, dst, send_sem, recv_sem, local_sem):
        for step in range(1, count):
            peer = lax.rem(me + step, count)
            pltpu.make_async_remote_copy(
                src_ref=src(peer),
                dst_ref=dst(me),
                send_sem=send_sem,
                recv_sem=recv_sem,
                device_id={axis: peer},
                device_id_type=MESH,
            ).start()
        pltpu.make_async_copy(src(me), dst(me), local_sem).start()

    def row_part(grid, h, k):
        c, q = where_of(k)
        return lambda p: grid.at[h, p, c, pl.ds(q * pair_depth, pair_depth)]

    def col_part(grid, h, k):
        c, q = where_of(k)
        return lambda j: grid.at[h, j, c, pl.ds(q * depth, depth)]

    def many(grid, h, k, count, size):
        c, q = where_of(k)
        return grid.at[h, pl.ds(0, count - 1), c, pl.ds(q * size, size)]

    def wait_bytes(ref, sem):
        pltpu.make_async_copy(ref, ref, sem).wait()

    def wait_row(grid, h, k, recv, local):
        n = h * chunks + k
        wait_bytes(many(grid, h, k, row_count, pair_depth), recv.at[n])
        wait_bytes(row_part(grid, h, k)(me_row), local.at[n])

    def wait_col(grid, h, k, recv, local):
        n = h * chunks + k
        wait_bytes(many(grid, h, k, col_count, depth), recv.at[n])
        wait_bytes(col_part(grid, h, k)(me_col), local.at[n])

    def send_row(src, dst, h, k, sems):
        n = h * chunks + k
        send("row", row_count, me_row, row_part(src, h, k), row_part(dst, h, k),
             sems[0].at[n], sems[1].at[n], sems[2].at[n])

    def send_col(src, dst, h, k, sems):
        n = h * chunks + k
        send("col", col_count, me_col, col_part(src, h, k), col_part(dst, h, k),
             sems[0].at[n], sems[1].at[n], sems[2].at[n])

    def ahead_lines(h, k):
        c, q = where_of(k)
        rows = []
        for zb in range(2):
            members = [
                jnp.concatenate(
                    [source[r, c, q * depth + 2 * z + zb] for z in range(pair_depth)], axis=0
                )
                for r in range(2)
            ]
            rows.append(jnp.concatenate(members, axis=1))
        result = right_product(
            jnp.concatenate(rows, axis=0), line_table[h, 0], line_table[h, 1], False
        )
        count = pair_depth * local_y
        for pp in range(row_count // 2):
            part = result[:, pp * LANES : (pp + 1) * LANES]
            first, second = swap_lanes(part[:count], part[count:])
            for b, value in ((0, first), (1, second)):
                grid_a[h, 2 * pp + b, c, pl.ds(q * pair_depth, pair_depth)] = value.reshape(
                    pair_depth, local_y, LANES
                )
        send_row(grid_a, grid_b, h, k, (f1s, f1r, f1l))

    def ahead_columns(h, k):
        c, q = where_of(k)
        wait_row(grid_b, h, k, f1r, f1l)

        def step(t, carry):
            z0 = q * pair_depth + 2 * t
            columns = [
                grid_b[h, :, c, z0 + i].reshape(row_count * local_y, LANES) for i in range(2)
            ]
            result = left_product(ahead_table[...], columns)
            for i in range(2):
                part = result[:, i * LANES : (i + 1) * LANES]
                part = part.reshape(col_count, 2, pairs_y, LANES)
                first, second = swap_lanes(part[:, 0], part[:, 1])
                grid_c[h, :, c, 2 * (z0 + i)] = first
                grid_c[h, :, c, 2 * (z0 + i) + 1] = second
            return carry

        lax.fori_loop(0, pair_depth // 2, step, 0)
        send_col(grid_c, grid_d, h, k, (f2s, f2r, f2l))

    def mix(h, unit):
        step = h * units + unit
        slot = step % 2
        ky = unit * 2
        flat = [
            [grid_d.at[h, j, c].reshape(local_z * pairs_y, LANES) for c in range(3)]
            for j in range(col_count)
        ]
        for c in range(3):
            columns = []
            for i in range(2):
                pieces = [
                    flat[j][c][pl.ds(ky + i, local_z, stride=pairs_y), :] for j in range(col_count)
                ]
                columns.append(jnp.concatenate(pieces, axis=0))
            mixed[c] = left_product(ahead_table[...], columns)
        for copy in green_copies(step):
            copy.wait()
        for entry in range(6):
            for i in range(2):
                first = green_slot[slot, 0, entry, i]
                second = green_slot[slot, 1, entry, i]
                block = jnp.concatenate([first, second, first, second], axis=0)
                weights[entry, :, i * LANES : (i + 1) * LANES] = block.T.astype(jnp.float32)

        @pl.when(step + 2 < 2 * units)
        def _():
            for copy in green_copies(step + 2):
                copy.start()

        for c in range(3):
            columns = []
            for i in range(2):
                part = slice(i * LANES, (i + 1) * LANES)
                total = None
                for other in range(3):
                    term = weights[tensor_pairs[c][other], :, part] * mixed[other, :, part]
                    total = term if total is None else total + term
                columns.append(total)
            result = left_product(back_table[...], columns)
            for i in range(2):
                for j in range(col_count):
                    flat[j][c][pl.ds(ky + i, local_z, stride=pairs_y), :] = result[
                        j * local_z : (j + 1) * local_z, i * LANES : (i + 1) * LANES
                    ]

    def mix_some(h, turn, turns):
        def step(unit, carry):
            mix(h, unit)
            return carry

        low = jnp.clip(turn, 0, turns) * units // turns
        lax.fori_loop(low, jnp.clip(turn + 1, 0, turns) * units // turns, step, 0)

    def back_columns(h, k):
        c, q = where_of(k)

        def step(t, carry):
            z0 = q * pair_depth + 2 * t
            columns = []
            for i in range(2):
                first, second = swap_lanes(
                    grid_c[h, :, c, 2 * (z0 + i)], grid_c[h, :, c, 2 * (z0 + i) + 1]
                )
                pieces = []
                for j in range(col_count):
                    pieces += [first[j], second[j]]
                columns.append(jnp.concatenate(pieces, axis=0))
            result = left_product(back_table[...], columns)
            for i in range(2):
                part = result[:, i * LANES : (i + 1) * LANES]
                grid_b[h, :, c, z0 + i] = part.reshape(row_count, local_y, LANES)
            return carry

        lax.fori_loop(0, pair_depth // 2, step, 0)
        send_row(grid_b, grid_a, h, k, (b2s, b2r, b2l))

    scaling = 1.0 / (4.0 * half_x * half_y * full_z)

    def back_lines(k):
        c, q = where_of(k)
        for h in range(2):
            wait_row(grid_a, h, k, b2r, b2l)
        count = pair_depth * local_y
        result = None
        for h in range(2):
            low, high = [], []
            for pp in range(row_count // 2):
                values = [
                    grid_a[h, 2 * pp + b, c, pl.ds(q * pair_depth, pair_depth)].reshape(count, LANES)
                    for b in range(2)
                ]
                first, second = swap_lanes(*values)
                low.append(first)
                high.append(second)
            rows = jnp.concatenate(
                [jnp.concatenate(low, axis=1), jnp.concatenate(high, axis=1)], axis=0
            )
            term = right_product(rows, line_table[h, 0], line_table[h, 1], True)
            result = term if result is None else result + term
        partial = [None] * (4 * blocks)
        for zb in range(2):
            for pair in range(pair_depth):
                z = q * depth + 2 * pair + zb
                start = zb * count + pair * local_y
                weight = chi_all[z] * scaling
                columns = []
                for r in range(2):
                    value = (
                        source[r, c, z]
                        - weight * result[start : start + local_y, r * half_x : (r + 1) * half_x]
                    )
                    image[r, c, z] = value
                    columns.append(value)
                for a in range(2 * blocks):
                    member = basis[a // 2, a % 2, c, z]
                    for r in range(2):
                        term = fold(member * columns[r])
                        old = partial[2 * a + r]
                        partial[2 * a + r] = term if old is None else old + term
        for i in range(4 * blocks):
            sums[i] = sums[i] + partial[i]

    def exchange(gather, n):
        def start(peer):
            pltpu.make_async_remote_copy(
                src_ref=gather.at[me],
                dst_ref=gather.at[me],
                send_sem=gather_send.at[n],
                recv_sem=gather_recv.at[n],
                device_id=peer,
                device_id_type=MESH,
            ).start()

        others(start)
        rest = gather.at[pl.ds(0, world - 1)]
        wait_bytes(rest, gather_recv.at[n])
        wait_bytes(rest, gather_send.at[n])
        total = gather[0]
        for i in range(1, world):
            total = total + gather[i]
        return jnp.sum(total, axis=1, keepdims=True) * (1.0 / (3.0 * chi_all.size * world))

    def orthonormalize():
        gather_one[me] = jnp.sum(sums[...], axis=1)
        products = exchange(gather_one, 0)
        coefficients[...] = jnp.broadcast_to(products, coefficients.shape)
        zero = jnp.zeros((8, LANES), jnp.float32)

        def project(z, totals):
            totals = list(totals)
            for c in range(3):
                columns = [image[r, c, z] for r in range(2)]
                for a in range(2 * blocks):
                    member = basis[a // 2, a % 2, c, z]
                    for r in range(2):
                        i = 2 * a + r
                        columns[r] = columns[r] - products[i : i + 1] * member
                for r in range(2):
                    image[r, c, z] = columns[r]
                for n, (i, j) in enumerate(((0, 0), (0, 1), (1, 1))):
                    totals[n] = totals[n] + fold(columns[i] * columns[j])
            return tuple(totals)

        totals = lax.fori_loop(0, local_z, project, (zero, zero, zero))
        for c in range(3):
            out_copy(c).start()
        rows = [jnp.sum(total, axis=0, keepdims=True) for total in totals]
        gather_two[me] = jnp.concatenate(rows + [zero[:5]], axis=0)
        gram = exchange(gather_two, 1)
        lead = jnp.sqrt(gram[0:1] + 1e-06)
        cross = gram[1:2] / lead
        tail = jnp.sqrt(gram[2:3] - cross * cross + 1e-06)
        none = zero[:1, :1]
        scales = [1.0 / lead, 1.0 / tail, none, -cross / lead / tail]
        values = jnp.concatenate([lead, cross, none, tail] + scales, axis=0)
        factor[...] = jnp.broadcast_to(values, factor.shape)
        for c in range(3):
            out_copy(c).wait()

    def fold(value):
        total = None
        for i in range(local_y // 8):
            for j in range(half_x // LANES):
                piece = value[i * 8 : (i + 1) * 8, j * LANES : (j + 1) * LANES]
                total = piece if total is None else total + piece
        return total

    def loop(body):
        def step(k, carry):
            body(k)
            return carry

        lax.fori_loop(0, chunks, step, 0)

    for c in range(3):
        source_copy(c).start()
    for i in range(2):
        for copy in green_copies(i):
            copy.start()
    chi_copy.start()
    older.start()
    build_line_table(0)
    sums[...] = jnp.zeros(sums.shape, jnp.float32)
    for c in range(3):
        source_copy(c).wait()
    pl.semaphore_wait(barrier, world - 1)
    def ahead_send(n):
        ahead_lines(n // chunks, n % chunks)

    def back_send(n):
        send_col(grid_d, grid_c, n // chunks, n % chunks, (b1s, b1r, b1l))

    for n in range(AHEAD):
        ahead_send(jnp.int32(n))
    build_left_tables()
    build_line_table(1)

    def free_rows(k):
        for h in range(2):
            wait_bytes(many(grid_a, h, k, row_count, pair_depth), f1s.at[h * chunks + k])

    def free_cols(h):
        loop(lambda k: wait_bytes(many(grid_c, h, k, col_count, depth), f2s.at[h * chunks + k]))
        for step in range(1, col_count):
            peer = lax.rem(me_col + step, col_count)
            pl.semaphore_signal(
                col_credit.at[h], 1, device_id={"col": peer}, device_id_type=MESH
            )

    def first_half(n, carry):
        ahead_columns(n // chunks, n % chunks)

        @pl.when(n + AHEAD < 2 * chunks)
        def _():
            ahead_send(n + AHEAD)

        @pl.when(n == chunks)
        def _():
            loop(lambda k: wait_col(grid_d, 0, k, f2r, f2l))

        mix_some(0, n - chunks, chunks - 1)
        return carry

    lax.fori_loop(0, 2 * chunks, first_half, 0)
    free_cols(0)
    pl.semaphore_wait(col_credit.at[0], col_count - 1)
    for n in range(AHEAD):
        back_send(jnp.int32(n))
    loop(free_rows)
    for step in range(1, row_count):
        peer = lax.rem(me_row + step, row_count)
        pl.semaphore_signal(row_credit, 1, device_id={"row": peer}, device_id_type=MESH)
    loop(lambda k: wait_col(grid_d, 1, k, f2r, f2l))
    free_cols(1)
    chi_copy.wait()
    older.wait()
    pl.semaphore_wait(row_credit, row_count - 1)
    pl.semaphore_wait(col_credit.at[1], col_count - 1)

    def second_half(n, carry):
        h, k = n // chunks, n % chunks
        wait_col(grid_c, h, k, b1r, b1l)

        @pl.when(n + AHEAD < 2 * chunks)
        def _():
            back_send(n + AHEAD)

        back_columns(h, k)
        mix_some(1, n, chunks - AHEAD)

        @pl.when(n >= chunks + LAG)
        def _():
            back_lines(n - chunks - LAG)

        return carry

    lax.fori_loop(0, 2 * chunks, second_half, 0)
    for k in range(chunks - LAG, chunks):
        back_lines(jnp.int32(k))
    orthonormalize()

    def finish(k):
        for h in range(2):
            n = h * chunks + k
            wait_bytes(many(grid_d, h, k, col_count, depth), b1s.at[n])
            wait_bytes(many(grid_b, h, k, row_count, pair_depth), b2s.at[n])

    loop(finish)


def fits_kernel(susceptibility, green_spectra):
    local_z, local_y, half_x = susceptibility.shape
    full_z, part_y, part_x = green_spectra.shape[1:]
    return (
        part_x == LANES // 2
        and part_y % 16 == 0
        and full_z % LANES == 0
        and full_z == 2 * local_y * lax.axis_size("row")
        and local_y % 8 == 0
        and local_z % (4 * SLABS) == 0
        and half_x % LANES == 0
        and lax.axis_size("row") % 2 == 0
    )


def fused_step(krylov_basis, susceptibility, green_spectra):
    row_count = lax.axis_size("row")
    col_count = lax.axis_size("col")
    world = row_count * col_count
    blocks = krylov_basis.shape[0]
    local_z, local_y, half_x = susceptibility.shape
    full_z, part_y, part_x = green_spectra.shape[1:]
    half_y = local_y * row_count
    pairs_y = part_y // 2
    row_grid = pltpu.VMEM((2, row_count, 3, local_z // 2, local_y, LANES), jnp.float32)
    col_grid = pltpu.VMEM((2, col_count, 3, local_z, pairs_y, LANES), jnp.float32)
    dma = pltpu.SemaphoreType.DMA
    whole = pl.BlockSpec(memory_space=pltpu.VMEM)
    outside = pl.BlockSpec(memory_space=pl.ANY)
    field = (2, 3, local_z, local_y, half_x)
    projected, coefficients, factor = pl.pallas_call(
        functools.partial(field_kernel, row_count, col_count),
        out_shape=(
            jax.ShapeDtypeStruct(field, jnp.float32),
            jax.ShapeDtypeStruct((4 * blocks, LANES), jnp.float32),
            jax.ShapeDtypeStruct((8, LANES), jnp.float32),
        ),
        in_specs=[outside] * 3,
        out_specs=(outside, whole, whole),
        scratch_shapes=[
            row_grid,
            row_grid,
            col_grid,
            col_grid,
            pltpu.VMEM((2, 2, 2 * half_x, row_count * part_x), jnp.bfloat16),
            pltpu.VMEM((2 * half_y, 6 * half_y), jnp.bfloat16),
            pltpu.VMEM((half_y, 12 * half_y), jnp.bfloat16),
            pltpu.VMEM((blocks,) + field, jnp.float32),
            pltpu.VMEM((local_z, local_y, half_x), jnp.float32),
            pltpu.VMEM(field, jnp.float32),
            pltpu.VMEM((2, 2, 6, 2, 32, full_z), jnp.bfloat16),
            pltpu.VMEM((6, full_z, 2 * LANES), jnp.float32),
            pltpu.VMEM((3, full_z, 2 * LANES), jnp.float32),
            pltpu.VMEM((4 * blocks, 8, LANES), jnp.float32),
            pltpu.VMEM((world, 4 * blocks, LANES), jnp.float32),
            pltpu.VMEM((world, 8, LANES), jnp.float32),
        ]
        + [dma((2 * 3 * SLABS,))] * 12
        + [
            dma((2, 2)),
            dma,
            dma((3,)),
            dma,
            dma((3,)),
            dma((2,)),
            dma((2,)),
            pltpu.SemaphoreType.REGULAR,
            pltpu.SemaphoreType.REGULAR((2,)),
        ],
        compiler_params=pltpu.CompilerParams(
            collective_id=0, has_side_effects=True, vmem_limit_bytes=67043328
        ),
        name="fused_step",
    )(krylov_basis, susceptibility, green_spectra.transpose(0, 2, 3, 1))
    projections = coefficients[:, 0].reshape(blocks, 2, 2)
    block_factor = factor[:4, 0].reshape(2, 2)
    scale = factor[4:6, 0].reshape(2, 1, 1, 1, 1)
    shift = factor[6:8, 0].reshape(2, 1, 1, 1, 1)
    return projections, projected * scale + projected[:1] * shift, block_factor


def total_over_devices(partial):
    return jnp.sum(lax.all_gather(partial, ("row", "col")), axis=0)


def per_device(krylov_basis, susceptibility, green_spectra):
    blocks = krylov_basis.shape[0]
    latest = krylov_basis[-1]
    if fits_kernel(susceptibility, green_spectra):
        return fused_step(krylov_basis, susceptibility, green_spectra)
    response = convolve(latest, green_spectra)
    image = [latest[:, c] - susceptibility[None] * response[c] for c in range(3)]
    image = jnp.stack(image, axis=1)
    entry_count = 3.0 * susceptibility.size * lax.axis_size("row") * lax.axis_size("col")
    basis = krylov_basis.reshape((2 * blocks,) + image.shape[1:])
    local_coeffs = jnp.stack(
        [jnp.sum(basis * image[j][None], axis=(1, 2, 3, 4)) for j in range(2)], axis=1
    )
    coefficients = total_over_devices(local_coeffs / entry_count)
    projected = []
    for j in range(2):
        column = image[j]
        for a in range(2 * blocks):
            column = column - coefficients[a, j] * basis[a]
        projected.append(column)
    g00 = jnp.sum(projected[0] * projected[0])
    g01 = jnp.sum(projected[0] * projected[1])
    g11 = jnp.sum(projected[1] * projected[1])
    gram = total_over_devices(jnp.stack([g00, g01, g11]) / entry_count)
    lead_norm = jnp.sqrt(gram[0] + 1e-06)
    cross_term = gram[1] / lead_norm
    tail_norm = jnp.sqrt(gram[2] - cross_term * cross_term + 1e-06)
    first_column = projected[0] / lead_norm
    second_column = (projected[1] - cross_term * first_column) / tail_norm
    next_block = jnp.stack([first_column, second_column])
    block_factor = jnp.stack(
        [jnp.stack([lead_norm, cross_term]), jnp.stack([jnp.zeros_like(lead_norm), tail_norm])]
    )
    return (coefficients.reshape(blocks, 2, 2), next_block, block_factor)


def solution(mesh):
    in_specs = (
        P(None, None, None, "col", "row", None),
        P("col", "row", None),
        P(None, None, "col", "row"),
    )
    out_specs = (P(), P(None, None, "col", "row", None), P())
    return jax.shard_map(
        per_device, mesh=mesh, in_specs=in_specs, out_specs=out_specs, check_vma=False
    )
```
